32 devices in a mesh: stage: 8 (over z, y), expert: 4 (over x, core).
Axes of the slice: x: 2, y: 2, z: 4, core: 2. Of those that a mesh axis runs over, the one named last changes fastest.
Arguments:
- x_acts: bfloat16 [2, 8, 4096, 512], P(None, 'stage', 'expert')
- expert_ids: int32 [2, 8, 4096, 2], P(None, 'stage', 'expert')
- gate_wts: float32 [2, 8, 4096, 2], P(None, 'stage', 'expert')
- w_in: bfloat16 [8, 8, 512, 1792], P('stage', 'expert')
- w_up: bfloat16 [8, 8, 512, 1792], P('stage', 'expert')
- w_out: bfloat16 [8, 8, 1792, 512], P('stage', 'expert')
- d_out: bfloat16 [8, 4096, 512], P('stage', 'expert')
Outputs:
- output 1: bfloat16 [8, 4096, 512], P('stage', 'expert')
- output 2: bfloat16 [8, 4096, 512], P('stage', 'expert')
- output 3: bfloat16 [8, 8, 512, 1792], P('stage', 'expert')
- output 4: bfloat16 [8, 8, 512, 1792], P('stage', 'expert')
- output 5: bfloat16 [8, 8, 1792, 512], P('stage', 'expert')
All inputs are finite; a program needn't handle non-finite values.
Results may differ from the reference program's by a relative error of at most 0.0011.
Values are sent between devices in bfloat16 or wider.
A program may use at most 1 GiB of HBM per device.

```python
import jax
import jax.numpy as jnp
from jax import lax

NUM_STAGES = 8
GROUP_SIZE = 4
TOKENS_DEV = 1024
MODEL_DIM = 512
FFN_DIM = 1792
NUM_EXPERTS = 8
TOP_K = 2
CAPACITY = 3 * TOP_K * TOKENS_DEV // (2 * NUM_EXPERTS)
SLOTS = NUM_EXPERTS * CAPACITY


def device_routing(dev_key):
    key_order, key_pos = jax.random.split(dev_key)
    block_expert = jax.random.permutation(key_order, NUM_EXPERTS)
    token_pos = jax.random.permutation(key_pos, TOKENS_DEV)
    spacing = TOKENS_DEV // TOP_K
    cold_len = TOKENS_DEV // (2 * NUM_EXPERTS)
    slot_pos = (token_pos[:, None] + spacing * jnp.arange(TOP_K)[None, :]) % TOKENS_DEV
    within = slot_pos % (4 * cold_len)
    block_idx = 2 * (slot_pos // (4 * cold_len)) + (within >= 3 * cold_len).astype(jnp.int32)
    return block_expert[block_idx].astype(jnp.int32)


def draw_routing(route_key):
    sub_keys = jax.random.split(route_key, 2 * NUM_STAGES * GROUP_SIZE)
    choices = jax.vmap(device_routing)(sub_keys)
    return choices.reshape(2, NUM_STAGES, GROUP_SIZE * TOKENS_DEV, TOP_K)


def setup_inputs(seed: int = 0) -> dict:
    sub_keys = jax.random.split(jax.random.key(seed), 7)
    tok_shape = (2, NUM_STAGES, GROUP_SIZE * TOKENS_DEV)
    w_shape = (NUM_STAGES, NUM_EXPERTS, MODEL_DIM, FFN_DIM)
    x_acts = jax.random.normal(sub_keys[0], tok_shape + (MODEL_DIM,), jnp.float32)
    expert_ids = draw_routing(sub_keys[1])
    gate_wts = jax.random.uniform(sub_keys[2], tok_shape + (TOP_K,), jnp.float32, 0.5, 1.5) / TOP_K
    w_in = jax.random.normal(sub_keys[3], w_shape, jnp.float32) * MODEL_DIM ** -0.5
    w_up = jax.random.normal(sub_keys[4], w_shape, jnp.float32) * MODEL_DIM ** -0.5
    w_out = jax.random.normal(sub_keys[5], (NUM_STAGES, NUM_EXPERTS, FFN_DIM, MODEL_DIM), jnp.float32) * FFN_DIM ** -0.5
    d_out = jax.random.normal(sub_keys[6], (NUM_STAGES, GROUP_SIZE * TOKENS_DEV, MODEL_DIM), jnp.float32)
    return dict(x_acts=x_acts.astype(jnp.bfloat16), expert_ids=expert_ids, gate_wts=gate_wts,
                w_in=w_in.astype(jnp.bfloat16), w_up=w_up.astype(jnp.bfloat16),
                w_out=w_out.astype(jnp.bfloat16), d_out=d_out.astype(jnp.bfloat16))


def bf16_cast(raw_value):
    return raw_value.astype(jnp.bfloat16).astype(jnp.float32)


def slot_index(choices):
    chosen = choices[:, :, None] == jnp.arange(NUM_EXPERTS)[None, None, :]
    taken = jnp.any(chosen, axis=1).astype(jnp.int32)
    slot_rank = jnp.cumsum(taken, axis=0) - 1
    return choices * CAPACITY + jnp.take_along_axis(slot_rank, choices, axis=1)


def gather_slots(slot_idx, gates):
    flat_idx = slot_idx.reshape(-1)
    owner = jnp.zeros((SLOTS,), jnp.int32).at[flat_idx].set(jnp.repeat(jnp.arange(TOKENS_DEV), TOP_K))
    slot_gate = jnp.zeros((SLOTS,), jnp.float32).at[flat_idx].set(gates.reshape(-1))
    return owner, slot_gate.reshape(NUM_EXPERTS, CAPACITY)


def stage_layer(stage_args):
    x_two, choice_two, gate_two, w_in_s, w_up_s, w_out_s, dy_stage = stage_args
    w_in_f = w_in_s.astype(jnp.float32)
    w_up_f = w_up_s.astype(jnp.float32)
    w_out_f = w_out_s.astype(jnp.float32)

    def per_device(tensor):
        return tensor.reshape((GROUP_SIZE, TOKENS_DEV) + tensor.shape[1:])

    def device_step(grad_acc, dev_block):
        x_fw, ch_fw, g_fw, x_bw, ch_bw, g_bw, dy_bw = dev_block
        idx_fw = slot_index(ch_fw)
        owner_fw, gate_fw = gather_slots(idx_fw, g_fw)
        rows_fw = x_fw.astype(jnp.float32)[owner_fw].reshape(NUM_EXPERTS, CAPACITY, MODEL_DIM)
        pre_in = jnp.einsum('ecd,edf->ecf', rows_fw, w_in_f)
        pre_up = jnp.einsum('ecd,edf->ecf', rows_fw, w_up_f)
        hidden = bf16_cast(jax.nn.silu(pre_in) * pre_up)
        expert_out = jnp.einsum('ecf,efd->ecd', hidden, w_out_f)
        contrib = bf16_cast(gate_fw[:, :, None] * expert_out).reshape(SLOTS, MODEL_DIM)
        y_dev = jnp.sum(contrib[idx_fw], axis=1).astype(jnp.bfloat16)

        idx_bw = slot_index(ch_bw)
        owner_bw, gate_bw = gather_slots(idx_bw, g_bw)
        rows_bw = x_bw.astype(jnp.float32)[owner_bw].reshape(NUM_EXPERTS, CAPACITY, MODEL_DIM)
        dy_rows = dy_bw.astype(jnp.float32)[owner_bw].reshape(NUM_EXPERTS, CAPACITY, MODEL_DIM)
        pre_in = jnp.einsum('ecd,edf->ecf', rows_bw, w_in_f)
        pre_up = jnp.einsum('ecd,edf->ecf', rows_bw, w_up_f)
        sig_in = jax.nn.sigmoid(pre_in)
        act_in = pre_in * sig_in
        hidden = bf16_cast(act_in * pre_up)
        gated_dy = bf16_cast(gate_bw[:, :, None] * dy_rows)
        d_hidden = jnp.einsum('ecd,efd->ecf', gated_dy, w_out_f)
        d_pre_in = bf16_cast(d_hidden * pre_up * sig_in * (1.0 + pre_in * (1.0 - sig_in)))
        d_pre_up = bf16_cast(d_hidden * act_in)
        dx_slot = bf16_cast(jnp.einsum('ecf,edf->ecd', d_pre_in, w_in_f) + jnp.einsum('ecf,edf->ecd', d_pre_up, w_up_f))
        dx_dev = jnp.sum(dx_slot.reshape(SLOTS, MODEL_DIM)[idx_bw], axis=1).astype(jnp.bfloat16)
        acc_in, acc_up, acc_out = grad_acc
        new_acc = (acc_in + jnp.einsum('ecd,ecf->edf', rows_bw, d_pre_in),
                   acc_up + jnp.einsum('ecd,ecf->edf', rows_bw, d_pre_up),
                   acc_out + jnp.einsum('ecf,ecd->efd', hidden, gated_dy))
        return new_acc, (y_dev, dx_dev)

    zero_acc = (jnp.zeros(w_in_s.shape, jnp.float32), jnp.zeros(w_up_s.shape, jnp.float32),
                jnp.zeros(w_out_s.shape, jnp.float32))
    blocks = (per_device(x_two[1]), per_device(choice_two[1]), per_device(gate_two[1]),
              per_device(x_two[0]), per_device(choice_two[0]), per_device(gate_two[0]),
              per_device(dy_stage))
    grads, outs = lax.scan(device_step, zero_acc, blocks)
    tok_total = GROUP_SIZE * TOKENS_DEV
    return (outs[0].reshape(tok_total, MODEL_DIM), outs[1].reshape(tok_total, MODEL_DIM),
            grads[0].astype(jnp.bfloat16), grads[1].astype(jnp.bfloat16), grads[2].astype(jnp.bfloat16))


def reference(x_acts, expert_ids, gate_wts, w_in, w_up, w_out, d_out):
    x_prev = jnp.moveaxis(jnp.roll(x_acts, 1, axis=1), 1, 0)
    ids_prev = jnp.moveaxis(jnp.roll(expert_ids, 1, axis=1), 1, 0)
    gate_prev = jnp.moveaxis(jnp.roll(gate_wts, 1, axis=1), 1, 0)
    y_out, dx_next, d_w_in, d_w_up, d_w_out = lax.map(
        stage_layer, (x_prev, ids_prev, gate_prev, w_in, w_up, w_out, d_out))
    d_x = jnp.roll(dx_next, -1, axis=0)
    return (y_out, d_x, d_w_in, d_w_up, d_w_out)
```

```python
import functools

import jax
import jax.numpy as jnp
from jax import lax
from jax.experimental import pallas as pl
from jax.experimental.pallas import tpu as pltpu
from jax.sharding import PartitionSpec as P

BF16 = jnp.bfloat16
F32 = jnp.float32
ROWS = 256
TILE = 256


def dot(lhs, rhs, lc=1, rc=0):
    return lax.dot_general(lhs, rhs, (((lc,), (rc,)), ((), ())), preferred_element_type=F32)


def routing_kernel(num_loc, meta_a, meta_b, meta_c, meta_d, pos_ref, gate_ref, cnt_ref):
    first = lax.axis_index('expert') * num_loc
    metas = (meta_a, meta_b, meta_c, meta_d)
    tokens = meta_a.shape[1]
    rows = num_loc * len(metas)
    lane = lax.broadcasted_iota(jnp.int32, (rows, tokens), 1)
    sub = lax.broadcasted_iota(jnp.int32, (rows, tokens), 0)
    expert = (first + sub // len(metas)).astype(F32)
    for mb in range(2):
        def field(idx):
            block = jnp.concatenate([m[4 * mb + idx:4 * mb + idx + 1, :] for m in metas], axis=0)
            return jnp.concatenate([block] * num_loc, axis=0)
        hit0, hit1 = field(0) == expert, field(1) == expert
        gate = jnp.where(hit0, field(2), 0.0) + jnp.where(hit1, field(3), 0.0)
        taken = jnp.where(hit0 | hit1, 1, 0)
        run = taken
        step = 1
        while step < tokens:
            run = run + jnp.where(lane >= step, pltpu.roll(run, step, 1), 0)
            step *= 2
        count = jnp.max(run, axis=1, keepdims=True) + jnp.zeros_like(run)
        before = jnp.where(sub % 2 == 1, pltpu.roll(count, 1, 0), 0)
        pos_ref[mb] = jnp.where(taken == 1, run - 1 + before, -1)
        gate_ref[mb] = gate
        cnt_ref[mb * rows:(mb + 1) * rows, :] = count[:, :128]


def route(metas, num_loc):
    tokens = metas[0].shape[1]
    rows = num_loc * len(metas)
    return pl.pallas_call(
        functools.partial(routing_kernel, num_loc),
        out_shape=(jax.ShapeDtypeStruct((2, rows, tokens), jnp.int32),
                   jax.ShapeDtypeStruct((2, rows, tokens), F32),
                   jax.ShapeDtypeStruct((2 * rows, 128), jnp.int32)),
        name='routing',
    )(*metas)


def start_weights(pairs, sems):
    for idx, (src, dst) in enumerate(pairs):
        for e in range(src.shape[0]):
            pltpu.make_async_copy(src.at[e], dst.at[e], sems.at[idx, e]).start()


def wait_weights(pairs, sems, e):
    for idx, (src, dst) in enumerate(pairs):
        pltpu.make_async_copy(src.at[e], dst.at[e], sems.at[idx, e]).wait()


def one_hot(pos_ref, row, base):
    tokens = pos_ref.shape[1]
    rid = lax.broadcasted_iota(jnp.int32, (ROWS, tokens), 0) + base
    return pos_ref[row:row + 1, :] == rid


def pick_gate(hits, gate_ref, rows):
    total = jnp.zeros((ROWS, 1), F32)
    for hit, row in zip(hits, rows):
        total += jnp.sum(jnp.where(hit, gate_ref[row:row + 1, :], 0.0), axis=1, keepdims=True)
    return total


def to_tokens(cnt, row_of, posc_ref, col_of, rows_ref, out_refs, cap):
    tokens = posc_ref.shape[0]
    num_loc = rows_ref.shape[0]
    for src, out_ref in enumerate(out_refs):
        width = cap if src == 0 else cap + 128

        def tile(m, carry):
            rows = pl.ds(pl.multiple_of(m * 256, 256), 256)
            total = None
            for e in range(num_loc):
                start = 0 if src == 0 else pl.multiple_of((cnt[row_of(e), 0] // 128) * 128, 128)
                lane = lax.broadcasted_iota(jnp.int32, (256, width), 1) + start
                hit = posc_ref[rows, col_of(e) + src:col_of(e) + src + 1] == lane
                part = dot(jnp.where(hit, 1.0, 0.0).astype(BF16), rows_ref[e, pl.ds(start, width), :])
                total = part if total is None else total + part
            out_ref[rows, :] = total.astype(BF16)
            return carry

        lax.fori_loop(0, tokens // 256, tile, 0)


def forward_kernel(mb, pair, num_loc, cap, cnt, pos_ref, gate_ref, posc_ref, xa_ref, xb_ref,
                   win_hbm, wup_hbm, wout_hbm, oa_ref, ob_ref, win, wup, wout, hid, rows_ref, sems):
    e, c = pl.program_id(0), pl.program_id(1)
    row_of = lambda ex: mb * num_loc * 4 + ex * 4 + 2 * pair
    weights = ((win_hbm, win), (wup_hbm, wup), (wout_hbm, wout))
    num_chunks = (cnt[row_of(e), 0] + cnt[row_of(e) + 1, 0] + ROWS - 1) // ROWS

    @pl.when((e == 0) & (c == 0))
    def _():
        start_weights(weights, sems)
        rows_ref[...] = jnp.zeros_like(rows_ref)

    @pl.when(c < num_chunks)
    def _():
        srow = 2 * pair
        hits = [one_hot(pos_ref.at[0, 0], srow + k, c * ROWS) for k in range(2)]
        gate = pick_gate(hits, gate_ref.at[0, 0], (srow, srow + 1))
        sel = [jnp.where(hit, 1.0, 0.0).astype(BF16) for hit in hits]
        x = (dot(sel[0], xa_ref[...]) + dot(sel[1], xb_ref[...])).astype(BF16)

        @pl.when(c == 0)
        def _():
            wait_weights(weights, sems, e)

        for t in range(win.shape[2] // TILE):
            cols = slice(t * TILE, (t + 1) * TILE)
            a = dot(x, win[e, :, cols])
            b = dot(x, wup[e, :, cols])
            hid[:, cols] = (a * jax.nn.sigmoid(a) * b).astype(BF16)
        out = dot(hid[...], wout[e])
        rows_ref[e, pl.ds(pl.multiple_of(c * ROWS, ROWS), ROWS), :] = (gate * out).astype(BF16)

    @pl.when((e == num_loc - 1) & (c == pl.num_programs(1) - 1))
    def _():
        to_tokens(cnt, row_of, posc_ref.at[0], lambda ex: ex * 4 + 2 * pair, rows_ref, (oa_ref, ob_ref), cap)


def backward_kernel(mb, pair, num_loc, cap, cnt, pos_ref, gate_ref, posc_ref, xa_ref, xb_ref, da_ref, db_ref,
                    win_hbm, wup_hbm, wout_hbm, oa_ref, ob_ref, gin_ref, gup_ref, hid_ref, xt_ref, qt_ref,
                    win, wup, wout, rows_ref, sems):
    e, c = pl.program_id(0), pl.program_id(1)
    row_of = lambda ex: mb * num_loc * 4 + ex * 4 + 2 * pair
    weights = ((win_hbm, win), (wup_hbm, wup), (wout_hbm, wout))
    num_chunks = (cnt[row_of(e), 0] + cnt[row_of(e) + 1, 0] + ROWS - 1) // ROWS

    @pl.when((e == 0) & (c == 0))
    def _():
        start_weights(weights, sems)
        rows_ref[...] = jnp.zeros_like(rows_ref)

    @pl.when(c < num_chunks)
    def _():
        srow = 2 * pair
        hits = [one_hot(pos_ref.at[0, 0], srow + k, c * ROWS) for k in range(2)]
        gate = pick_gate(hits, gate_ref.at[0, 0], (srow, srow + 1))
        sel = [jnp.where(hit, 1.0, 0.0).astype(BF16) for hit in hits]
        x = (dot(sel[0], xa_ref[...]) + dot(sel[1], xb_ref[...]))
        dy = (dot(sel[0], da_ref[...]) + dot(sel[1], db_ref[...]))
        gdy = gate * dy
        xt_ref[0] = x.T.astype(BF16)
        qt_ref[0] = gdy.T.astype(BF16)
        x = x.astype(BF16)
        q = gdy.astype(BF16)

        @pl.when(c == 0)
        def _():
            wait_weights(weights, sems, e)

        for t in range(win.shape[2] // TILE):
            cols = slice(t * TILE, (t + 1) * TILE)
            a = dot(x, win[e, :, cols])
            b = dot(x, wup[e, :, cols])
            u = dot(q, wout[e, cols, :], 1, 1)
            sig = jax.nn.sigmoid(a)
            act = a * sig
            hid_ref[0, :, cols] = (act * b).astype(BF16)
            gin_ref[0, :, cols] = (u * b * sig * (1.0 + a * (1.0 - sig))).astype(BF16)
            gup_ref[0, :, cols] = (u * act).astype(BF16)
        out = dot(gin_ref[0], win[e], 1, 1) + dot(gup_ref[0], wup[e], 1, 1)
        rows_ref[e, pl.ds(pl.multiple_of(c * ROWS, ROWS), ROWS), :] = out.astype(BF16)

    @pl.when((e == num_loc - 1) & (c == pl.num_programs(1) - 1))
    def _():
        to_tokens(cnt, row_of, posc_ref.at[0], lambda ex: ex * 4 + 2 * pair, rows_ref, (oa_ref, ob_ref), cap)


def expert_call(kind, mb, pair, cap, cnt, pos, gate, posc, toks, w_in, w_up, w_out):
    num_loc, model, width = w_in.shape
    tokens = toks[0].shape[0]
    max_chunks = -(-2 * cap // ROWS)
    pad_rows = max_chunks * ROWS + 128
    row_of = lambda ex: mb * num_loc * 4 + ex * 4 + 2 * pair

    def clamp(e, c, cnt):
        return jnp.minimum(c, (cnt[row_of(e), 0] + cnt[row_of(e) + 1, 0] + ROWS - 1) // ROWS - 1)

    whole = lambda e, c, cnt: (0, 0)
    route_spec = pl.BlockSpec((1, 1, 4, tokens), lambda e, c, cnt: (mb, e, 0, 0))
    in_specs = [route_spec, route_spec,
                pl.BlockSpec((1, tokens, num_loc * 4), lambda e, c, cnt: (mb, 0, 0))]
    in_specs += [pl.BlockSpec((tokens, model), whole)] * len(toks)
    in_specs += [pl.BlockSpec(memory_space=pl.ANY)] * 3
    out_specs = [pl.BlockSpec((tokens, model), whole)] * 2
    out_shape = [jax.ShapeDtypeStruct((tokens, model), BF16)] * 2
    scratch = [pltpu.VMEM((num_loc, model, width), BF16), pltpu.VMEM((num_loc, model, width), BF16),
               pltpu.VMEM((num_loc, width, model), BF16)]
    if kind == 'fwd':
        body = forward_kernel
        scratch.append(pltpu.VMEM((ROWS, width), BF16))
    else:
        body = backward_kernel
        out_specs += [pl.BlockSpec((1, ROWS, width), lambda e, c, cnt: (e, clamp(e, c, cnt), 0))] * 3
        out_shape += [jax.ShapeDtypeStruct((num_loc, max_chunks * ROWS, width), BF16)] * 3
        out_specs += [pl.BlockSpec((1, model, ROWS), lambda e, c, cnt: (e, 0, clamp(e, c, cnt)))] * 2
        out_shape += [jax.ShapeDtypeStruct((num_loc, model, max_chunks * ROWS), BF16)] * 2
    scratch += [pltpu.VMEM((num_loc, pad_rows, model), BF16), pltpu.SemaphoreType.DMA((3, num_loc))]
    units = 3 if kind == 'fwd' else 5
    return pl.pallas_call(
        functools.partial(body, mb, pair, num_loc, cap),
        grid_spec=pltpu.PrefetchScalarGridSpec(
            num_scalar_prefetch=1, grid=(num_loc, max_chunks), in_specs=in_specs, out_specs=out_specs,
            scratch_shapes=scratch),
        out_shape=out_shape,
        compiler_params=pltpu.CompilerParams(dimension_semantics=('arbitrary', 'arbitrary')),
        cost_estimate=pl.CostEstimate(flops=units * 2 * num_loc * 2 * cap * model * width,
                                      bytes_accessed=20 * 2 ** 20, transcendentals=0),
        name=f'{kind}_pair{pair}',
    )(cnt, pos, gate, posc, *toks, w_in, w_up, w_out)


def weight_kernel(mb, num_loc, max_chunks, cnt, xt_l, qt_l, gin_l, gup_l, hid_l, xt_r, qt_r, gin_r, gup_r, hid_r,
                  din_ref, dup_ref, dout_ref, acc):
    e = pl.program_id(0)
    row_of = lambda ex: mb * num_loc * 4 + ex * 4

    def chunks(pair):
        row = row_of(e) + 2 * pair
        return (cnt[row, 0] + cnt[row + 1, 0] + ROWS - 1) // ROWS

    for n in range(1, max_chunks + 1):
        @pl.when(chunks(0) == n)
        def _(n=n):
            k = slice(0, n * ROWS)
            acc[0] = dot(xt_l[0, :, k], gin_l[0, k, :])
            acc[1] = dot(xt_l[0, :, k], gup_l[0, k, :])
            acc[2] = dot(qt_l[0, :, k], hid_l[0, k, :])

    for n in range(1, max_chunks + 1):
        @pl.when(chunks(1) == n)
        def _(n=n):
            k = slice(0, n * ROWS)
            din_ref[0] = (acc[0] + dot(xt_r[0, :, k], gin_r[0, k, :])).astype(BF16)
            dup_ref[0] = (acc[1] + dot(xt_r[0, :, k], gup_r[0, k, :])).astype(BF16)
            dout_ref[0] = (acc[2] + dot(qt_r[0, :, k], hid_r[0, k, :])).T.astype(BF16)


def weight_call(mb, cnt, left, right):
    num_loc, rows, width = left[2].shape
    model = left[0].shape[1]
    max_chunks = rows // ROWS
    tall = pl.BlockSpec((1, model, rows), lambda e, t, cnt: (e, 0, 0))
    wide = pl.BlockSpec((1, rows, TILE), lambda e, t, cnt: (e, 0, t))
    return pl.pallas_call(
        functools.partial(weight_kernel, mb, num_loc, max_chunks),
        grid_spec=pltpu.PrefetchScalarGridSpec(
            num_scalar_prefetch=1, grid=(num_loc, width // TILE),
            in_specs=[tall, tall, wide, wide, wide] * 2,
            out_specs=[pl.BlockSpec((1, model, TILE), lambda e, t, cnt: (e, 0, t))] * 2
            + [pl.BlockSpec((1, TILE, model), lambda e, t, cnt: (e, t, 0))],
            scratch_shapes=[pltpu.VMEM((3, model, TILE), F32)]),
        out_shape=[jax.ShapeDtypeStruct((num_loc, model, width), BF16)] * 2
        + [jax.ShapeDtypeStruct((num_loc, width, model), BF16)],
        compiler_params=pltpu.CompilerParams(dimension_semantics=('arbitrary', 'arbitrary')),
        cost_estimate=pl.CostEstimate(flops=12 * num_loc * rows * model * width,
                                      bytes_accessed=50 * 2 ** 20, transcendentals=0),
        name='weight_grads',
    )(cnt, *left, *right)


def solution(mesh):
    group = mesh.shape['expert']
    stages = mesh.shape['stage']
    axes = ('stage', 'expert')

    def move(arr, stage_step, flip):
        perm = [(s * group + i, ((s + stage_step) % stages) * group + (i ^ flip))
                for s in range(stages) for i in range(group)]
        return lax.ppermute(arr, axes, perm)

    def device_fn(x_acts, expert_ids, gate_wts, w_in, w_up, w_out, d_out):
        num_loc = w_in.shape[1]
        tokens = x_acts.shape[2]
        top_k = expert_ids.shape[3]
        cap = 3 * top_k * tokens // (2 * num_loc * group)
        wi, wu, wo = w_in[0], w_up[0], w_out[0]

        meta = jnp.concatenate([expert_ids[:, 0].astype(F32), gate_wts[:, 0]], axis=-1)
        meta = jnp.swapaxes(meta, 1, 2).reshape(2 * 2 * top_k, tokens)
        metas = [move(meta, 1, flip) for flip in range(4)]

        def gather(own):
            partner = move(own, 0, 1)
            other = move(own, 0, 2)
            return own, partner, other, move(other, 0, 1)

        def combine(r0, r1, r2, r3):
            r2 = (r2.astype(F32) + move(r3, 0, 1).astype(F32)).astype(BF16)
            total = r0.astype(F32) + move(r1, 0, 1).astype(F32) + move(r2, 0, 2).astype(F32)
            return total.astype(BF16)

        dy = gather(d_out[0])
        xb = gather(move(x_acts[0, 0], 1, 0))
        xf = gather(move(x_acts[1, 0], 1, 0))

        pos, gate, cnt = route(metas, num_loc)
        posc = jnp.swapaxes(pos, 1, 2)
        pos = pos.reshape(2, num_loc, 4, tokens)
        gate = gate.reshape(2, num_loc, 4, tokens)

        def call(kind, mb, pair, toks):
            return expert_call(kind, mb, pair, cap, cnt, pos, gate, posc, toks, wi, wu, wo)

        bl = call('bwd', 0, 0, (xb[0], xb[1], dy[0], dy[1]))
        br = call('bwd', 0, 1, (xb[2], xb[3], dy[2], dy[3]))
        dx = move(combine(bl[0], bl[1], br[0], br[1]), -1, 0)
        fr = call('fwd', 1, 1, (xf[2], xf[3]))
        fl = call('fwd', 1, 0, (xf[0], xf[1]))
        y = combine(fl[0], fl[1], fr[0], fr[1])

        def grads(res):
            gin, gup, hid, xt, qt = res[2:]
            return xt, qt, gin, gup, hid

        d_in, d_up, d_wout = weight_call(0, cnt, grads(bl), grads(br))
        return y[None], dx[None], d_in[None], d_up[None], d_wout[None]

    tok_spec = P(None, 'stage', 'expert', None)
    w_spec = P('stage', 'expert', None, None)
    row_spec = P('stage', 'expert', None)
    return jax.shard_map(device_fn, mesh=mesh,
                         in_specs=(tok_spec, tok_spec, tok_spec, w_spec, w_spec, w_spec, row_spec),
                         out_specs=(row_spec, row_spec, w_spec, w_spec, w_spec), check_vma=False)
```

```python
import functools

import jax
import jax.numpy as jnp
from jax import lax
from jax.experimental import pallas as pl
from jax.experimental.pallas import tpu as pltpu
from jax.sharding import PartitionSpec as P

BF16 = jnp.bfloat16
F32 = jnp.float32
MESH = pl.DeviceIdType.MESH
TILE = 256
PARTS = 4
EARLY = 2
A, B, A_FAR, B_FAR = range(4)


def dot(lhs, rhs, lc=1, rc=0):
    return lax.dot_general(lhs, rhs, (((lc,), (rc,)), ((), ())), preferred_element_type=F32)


def routing(mb, num_loc, ids, gates, pos, gate_rows, pos_cols):
    first = lax.axis_index('expert') * num_loc
    tokens = ids.shape[-1]
    rows = 4 * num_loc
    lane = lax.broadcasted_iota(jnp.int32, (rows, tokens), 1)
    sub = lax.broadcasted_iota(jnp.int32, (rows, tokens), 0)
    expert = first + sub % num_loc

    def field(ref, k):
        return jnp.concatenate([ref[s, mb, k:k + 1, :] for s in range(4) for _ in range(num_loc)], axis=0)

    hit0, hit1 = field(ids, 0) == expert, field(ids, 1) == expert
    gate_rows[mb] = jnp.where(hit0, field(gates, 0), 0.0) + jnp.where(hit1, field(gates, 1), 0.0)
    taken = jnp.where(hit0 | hit1, 1, 0)
    run = taken
    step = 1
    while step < tokens:
        run = run + jnp.where(lane >= step, pltpu.roll(run, step, 1), 0)
        step *= 2
    slot = jnp.where(taken == 1, run - 1, -1)
    pos[mb] = slot
    pos_cols[mb, :, 0:rows] = slot.T


def pick(pos, gate_rows, mb, row, cap):
    tokens = pos.shape[-1]
    hit = pos[mb, pl.ds(row, 1), :] == lax.broadcasted_iota(jnp.int32, (cap, tokens), 0)
    gate = jnp.sum(jnp.where(hit, gate_rows[mb, pl.ds(row, 1), :], 0.0), axis=1, keepdims=True)
    return jnp.where(hit, 1.0, 0.0).astype(BF16), gate


def to_tokens(pos_cols, mb, block, rows, out, done):
    num_loc, cap, _ = rows.shape
    part = out.shape[2] // PARTS
    for m in range(PARTS):
        span = slice(m * part, (m + 1) * part)
        cols = pltpu.roll(pos_cols[mb, span, :], lax.rem(128 - num_loc * block, 128), 1)
        slot = lax.broadcasted_iota(jnp.int32, (part, cap), 1)
        sel = [jnp.where(cols[:, e:e + 1] == slot, 1.0, 0.0).astype(BF16) for e in range(num_loc)]
        total = dot(jnp.concatenate(sel, axis=1), rows[...].reshape(num_loc * cap, rows.shape[2]))
        out[mb, block, span, :] = total.astype(BF16)
        done(m)


def add_bf16(*refs):
    total = refs[0][...].astype(F32)
    for ref in refs[1:]:
        total += ref[...].astype(F32)
    return total.astype(BF16)


def stage_kernel(num_stages, cap, ids_in, gates_in, x_hbm, dy_hbm, win_hbm, wup_hbm, wout_hbm,
                 dx_hbm, y_hbm, yx_hbm, wide_hbm, tall_hbm,
                 ids, gates, xs, dys, win, wup, wout, pos, gate_rows, pos_cols, rows, ret, rin, cin,
                 wide_buf, tall_buf, q_early, u_early,
                 meta_send, meta_recv, hop_send, hop_recv, fwd_send, fwd_recv, dy_sem, dy_send, dy_recv,
                 ret_send, ret_recv, crs_send, crs_recv, w_sem, out_sem, res_sem, pace):
    stage, me = lax.axis_index('stage'), lax.axis_index('expert')
    nxt, prv = lax.rem(stage + 1, num_stages), lax.rem(stage + num_stages - 1, num_stages)
    core, chip = lax.rem(me, 2), me // 2
    other = 1 - core

    def peer(flip):
        new_core = other if flip % 2 else core
        new_chip = 1 - chip if flip // 2 else chip
        return 2 * new_chip + new_core

    partner, across = (stage, peer(1)), (stage, peer(2))
    num_loc, model, width = win.shape
    tokens = xs.shape[2]
    part = tokens // PARTS
    tiles = width // TILE

    def remote(src, dst, send, recv, device):
        return pltpu.make_async_remote_copy(src_ref=src, dst_ref=dst, send_sem=send, recv_sem=recv,
                                            device_id=device, device_id_type=MESH)

    def meta(flip, k, block=None):
        src, dst = ((ids_in, ids), (gates_in, gates))[k]
        block = 2 * (flip // 2) + core if block is None else block
        return remote(src, dst.at[block], meta_send.at[k, flip], meta_recv.at[k, block], (nxt, peer(flip)))

    def piece(mb, block, k):
        return xs.at[mb, block, pl.ds(k * part, part)]

    def hop(mb, k):
        src = x_hbm.at[mb, 0, pl.ds(k * part, part)]
        return remote(src, piece(mb, core, k), hop_send.at[mb, k], hop_recv.at[mb, k], (nxt, me))

    def near(mb, k, block=None):
        ref = piece(mb, core if block is None else block, k)
        return remote(ref, ref, fwd_send.at[mb, 0, k], fwd_recv.at[mb, 0, k], partner)

    def cross(mb, k):
        return remote(piece(mb, core, k), piece(mb, 2 + core, k), fwd_send.at[mb, 1, k], fwd_recv.at[mb, 1, k],
                      across)

    def far(mb, k, block=None):
        ref = piece(mb, 2 + core if block is None else block, k)
        return remote(ref, ref, fwd_send.at[mb, 2, k], fwd_recv.at[mb, 2, k], partner)

    def near_arrived(mb):
        for k in range(PARTS):
            near(mb, k, other).wait_recv()

    def far_arrived(mb):
        for k in range(PARTS):
            far(mb, k, 2 + other).wait_recv()

    dy_own = pltpu.make_async_copy(dy_hbm.at[0], dys.at[core], dy_sem)
    dy_near = remote(dy_hbm.at[0], dys.at[core], dy_send.at[0], dy_recv.at[0], partner)
    dy_near_in = remote(dy_hbm.at[0], dys.at[other], dy_send.at[0], dy_recv.at[0], partner)
    dy_cross = remote(dy_hbm.at[0], dys.at[2 + core], dy_send.at[1], dy_recv.at[1], across)
    dy_far = remote(dys.at[2 + core], dys.at[2 + core], dy_send.at[2], dy_recv.at[2], partner)
    dy_far_in = remote(dys.at[2 + other], dys.at[2 + other], dy_send.at[2], dy_recv.at[2], partner)

    def back(mb, k, m, block=None):
        rows_m = pl.ds(m * part, part)
        src = ret.at[mb, 2 * k + other if block is None else block, rows_m]
        return remote(src, rin.at[mb, k, rows_m], ret_send.at[mb, k, m], ret_recv.at[mb, k, m], partner)

    def back_arrived(mb, k):
        for m in range(PARTS):
            back(mb, k, m).wait_recv()

    def send_back(mb, block):
        def done(m):
            @pl.when(lax.rem(block, 2) != core)
            def _():
                back(mb, block // 2, m, block).start()
        return done

    dx_cross = remote(ret.at[0, 2 + core], cin, crs_send, crs_recv, across)

    def dx_across():
        back_arrived(0, 1)
        ret[0, 2 + core] = add_bf16(ret.at[0, 2 + core], rin.at[0, 1])
        dx_cross.start()

    dx_save = pltpu.make_async_copy(ret.at[0, core], dx_hbm, res_sem.at[0])
    y_save = pltpu.make_async_copy(ret.at[1, core], y_hbm, res_sem.at[1])
    yx_save = pltpu.make_async_copy(ret.at[1, 2 + core], yx_hbm, res_sem.at[2])

    weights = [pltpu.make_async_copy(src.at[0], dst, w_sem.at[k])
               for k, (src, dst) in enumerate(((win_hbm, win), (wup_hbm, wup), (wout_hbm, wout)))]

    def outs(st):
        slot = lax.rem(st, 2)
        block, e = st // num_loc, lax.rem(st, num_loc)
        span = pl.ds(pl.multiple_of(block * cap, cap), cap)
        return (pltpu.make_async_copy(wide_buf.at[slot], wide_hbm.at[e, :, :, span], out_sem.at[slot, 0]),
                pltpu.make_async_copy(tall_buf.at[slot], tall_hbm.at[e, :, :, span], out_sem.at[slot, 1]))

    def at(now, when, on_core=None):
        cond = now == when if on_core is None else (now == when) & (core == on_core)
        return pl.when(cond)

    barrier = pltpu.get_barrier_semaphore()
    for device in [(prv, peer(flip)) for flip in range(4)] + [partner, across]:
        pl.semaphore_signal(barrier, inc=1, device_id=device, device_id_type=MESH)
    pl.semaphore_wait(barrier, 6)

    for flip in range(4):
        for k in range(2):
            meta(flip, k).start()

    @pl.when(core == 0)
    def _():
        for k in range(PARTS):
            hop(0, k).start()
        dy_cross.start()

    dy_near.start()
    dy_own.start()
    for copy in weights:
        copy.start()

    for block in range(4):
        for k in range(2):
            meta(0, k, block).wait_recv()
    for mb in range(2):
        routing(mb, num_loc, ids, gates, pos, gate_rows, pos_cols)
    dy_own.wait()
    dy_near_in.wait_recv()
    for copy in weights:
        copy.wait()

    def cotangent(st):
        sel, gate = pick(pos, gate_rows, 0, st, cap)
        return sel, gate * dot(sel, dys[st // num_loc])

    def early_step(st, carry):
        q = cotangent(st)[1].astype(BF16)
        q_early[st] = q
        for t in range(tiles):
            cols = slice(t * TILE, (t + 1) * TILE)
            u_early[st, :, cols] = dot(q, wout[lax.rem(st, num_loc), cols, :], 1, 1)
        return carry

    lax.fori_loop(0, EARLY, early_step, 0)

    @pl.when(core == 0)
    def _():
        for k in range(PARTS):
            hop(0, k).wait_recv()
            near(0, k).start()
            cross(0, k).start()
            if k == PARTS - 2:
                pl.semaphore_signal(pace, inc=1, device_id=partner, device_id_type=MESH)

    @pl.when(core == 1)
    def _():
        pl.semaphore_wait(pace, 1)
        for k in range(PARTS):
            hop(0, k).start()
        dy_cross.start()
        near_arrived(0)

    steps = 4 * num_loc
    half, most = PARTS // 2, PARTS - 1

    def pass_on(mb, lo, hi):
        for k in range(lo, hi):
            hop(mb, k).wait_recv()
            near(mb, k).start()
            cross(mb, k).start()

    def pass_far(mb, lo, hi):
        for k in range(lo, hi):
            cross(mb, k).wait_recv()
            far(mb, k).start()

    def backward_step(early, st, carry):
        block, e = st // num_loc, lax.rem(st, num_loc)
        slot = lax.rem(st, 2)

        @at(st, 1, on_core=1)
        def _():
            pass_on(0, 0, most)

        @at(st, num_loc, on_core=1)
        def _():
            pass_on(0, most, PARTS)

        @at(st, num_loc, on_core=0)
        def _():
            for k in range(PARTS):
                hop(1, k).start()
            near_arrived(0)

        @at(st, num_loc + 1, on_core=0)
        def _():
            dy_cross.wait_recv()
            dy_far.start()
            pass_far(0, 0, PARTS)

        @at(st, 2 * num_loc, on_core=0)
        def _():
            pass_on(1, 0, half)

        @at(st, 2 * num_loc, on_core=1)
        def _():
            for k in range(PARTS):
                hop(1, k).start()
            far_arrived(0)
            dy_far_in.wait_recv()

        @at(st, 2 * num_loc + 1, on_core=0)
        def _():
            pass_on(1, half, PARTS)

        @at(st, 2 * num_loc + 1, on_core=1)
        def _():
            dy_cross.wait_recv()
            dy_far.start()
            pass_far(0, 0, most)

        @at(st, 3 * num_loc, on_core=1)
        def _():
            pass_far(0, most, PARTS)
            pass_on(1, 0, half)

        @at(st, 3 * num_loc, on_core=0)
        def _():
            far_arrived(0)
            dy_far_in.wait_recv()

        @at(st, 3 * num_loc + 1, on_core=1)
        def _():
            pass_on(1, half, PARTS)

        @at(st, 3 * num_loc + 1, on_core=0)
        def _():
            dx_across()

        @pl.when(st >= 2)
        def _():
            for copy in outs(st - 2):
                copy.wait()

        if early:
            sel = pick(pos, gate_rows, 0, st, cap)[0]
            gdy = q_early[st].astype(F32)
        else:
            sel, gdy = cotangent(st)
        x = dot(sel, xs[0, block])
        tall_buf[slot, 0] = x.T.astype(BF16)
        tall_buf[slot, 1] = gdy.T.astype(BF16)
        x, q = x.astype(BF16), gdy.astype(BF16)
        for t in range(tiles):
            cols = slice(t * TILE, (t + 1) * TILE)
            a = dot(x, win[e, :, cols])
            b = dot(x, wup[e, :, cols])
            u = u_early[st, :, cols] if early else dot(q, wout[e, cols, :], 1, 1)
            sig = jax.nn.sigmoid(a)
            act = a * sig
            wide_buf[slot, t, 0] = (u * b * sig * (1.0 + a * (1.0 - sig))).astype(BF16)
            wide_buf[slot, t, 1] = (u * act).astype(BF16)
            wide_buf[slot, t, 2] = (act * b).astype(BF16)
        g_in = jnp.concatenate([wide_buf[slot, t, 0] for t in range(tiles)], axis=1)
        g_up = jnp.concatenate([wide_buf[slot, t, 1] for t in range(tiles)], axis=1)
        rows[e] = (dot(g_in, win[e], 1, 1) + dot(g_up, wup[e], 1, 1)).astype(BF16)
        for copy in outs(st):
            copy.start()

        @pl.when(e == num_loc - 1)
        def _():
            to_tokens(pos_cols, 0, block, rows, ret, send_back(0, block))

        return carry

    lax.fori_loop(0, EARLY, functools.partial(backward_step, True), 0)
    lax.fori_loop(EARLY, steps, functools.partial(backward_step, False), 0)
    for st in (steps - 2, steps - 1):
        for copy in outs(st):
            copy.wait()

    def forward_step(st, carry):
        block, e = st // num_loc, lax.rem(st, num_loc)

        @at(st, 0, on_core=1)
        def _():
            near_arrived(1)

        @at(st, 1, on_core=1)
        def _():
            dx_across()

        @at(st, num_loc, on_core=0)
        def _():
            near_arrived(1)

        @at(st, num_loc + 1, on_core=0)
        def _():
            pass_far(1, 0, PARTS)

        @at(st, 2 * num_loc, on_core=1)
        def _():
            far_arrived(1)

        @at(st, 2 * num_loc + 1, on_core=1)
        def _():
            pass_far(1, 0, most)

        @at(st, 3 * num_loc, on_core=1)
        def _():
            pass_far(1, most, PARTS)

        @at(st, 3 * num_loc)
        def _():
            back_arrived(1, 0)
            ret[1, core] = add_bf16(ret.at[1, core], rin.at[1, 0])
            y_save.start()

        @at(st, 3 * num_loc, on_core=0)
        def _():
            far_arrived(1)

        sel, gate = pick(pos, gate_rows, 1, st, cap)
        x = dot(sel, xs[1, block]).astype(BF16)
        for t in range(tiles):
            cols = slice(t * TILE, (t + 1) * TILE)
            a = dot(x, win[e, :, cols])
            b = dot(x, wup[e, :, cols])
            wide_buf[0, t, 0] = (a * jax.nn.sigmoid(a) * b).astype(BF16)
        hid = jnp.concatenate([wide_buf[0, t, 0] for t in range(tiles)], axis=1)
        rows[e] = (gate * dot(hid, wout[e])).astype(BF16)

        @pl.when(e == num_loc - 1)
        def _():
            to_tokens(pos_cols, 1, block, rows, ret, send_back(1, block))

        return carry

    lax.fori_loop(0, steps, forward_step, 0)
    back_arrived(1, 1)
    ret[1, 2 + core] = add_bf16(ret.at[1, 2 + core], rin.at[1, 1])
    yx_save.start()
    back_arrived(0, 0)
    dx_cross.wait_recv()
    ret[0, core] = add_bf16(ret.at[0, core], rin.at[0, 0], cin)
    dx_save.start()

    for flip in range(4):
        for k in range(2):
            meta(flip, k).wait_send()
    for mb in range(2):
        for k in range(PARTS):
            hop(mb, k).wait_send()
            near(mb, k).wait_send()
            cross(mb, k).wait_send()
            far(mb, k).wait_send()
            for j in range(2):
                back(mb, j, k).wait_send()
    for copy in (dy_near, dy_cross, dy_far, dx_cross):
        copy.wait_send()
    for copy in (y_save, yx_save, dx_save):
        copy.wait()


def stage_call(num_stages, cap, ids, gates, x_acts, d_out, w_in, w_up, w_out):
    _, num_loc, model, width = w_in.shape
    tokens = x_acts.shape[2]
    slots = 4 * cap
    whole = pl.BlockSpec(memory_space=pltpu.VMEM)
    anyspace = pl.BlockSpec(memory_space=pl.ANY)
    block = jax.ShapeDtypeStruct((tokens, model), BF16)
    wide = jax.ShapeDtypeStruct((num_loc, width // TILE, 3, slots, TILE), BF16)
    tall = jax.ShapeDtypeStruct((num_loc, 2, model, slots), BF16)
    vmem = pltpu.VMEM
    dma = pltpu.SemaphoreType.DMA
    return pl.pallas_call(
        functools.partial(stage_kernel, num_stages, cap),
        out_shape=[block] * 3 + [wide, tall],
        in_specs=[whole] * 2 + [anyspace] * 5,
        out_specs=[anyspace] * 5,
        scratch_shapes=[
            vmem((4,) + ids.shape, jnp.int32), vmem((4,) + gates.shape, F32),
            vmem((2, 4, tokens, model), BF16), vmem((4, tokens, model), BF16),
            vmem((num_loc, model, width), BF16), vmem((num_loc, model, width), BF16),
            vmem((num_loc, width, model), BF16),
            vmem((2, 4 * num_loc, tokens), jnp.int32), vmem((2, 4 * num_loc, tokens), F32),
            vmem((2, tokens, 128), jnp.int32),
            vmem((num_loc, cap, model), BF16), vmem((2, 4, tokens, model), BF16),
            vmem((2, 2, tokens, model), BF16), vmem((tokens, model), BF16),
            vmem((2, width // TILE, 3, cap, TILE), BF16), vmem((2, 2, model, cap), BF16),
            vmem((EARLY, cap, model), BF16), vmem((EARLY, cap, width), F32),
            dma((2, 4)), dma((2, 4)), dma((2, PARTS)), dma((2, PARTS)), dma((2, 3, PARTS)), dma((2, 3, PARTS)),
            dma, dma((3,)), dma((3,)), dma((2, 2, PARTS)), dma((2, 2, PARTS)), dma, dma, dma((3,)), dma((2, 2)), dma((3,)),
            pltpu.SemaphoreType.REGULAR,
        ],
        compiler_params=pltpu.CompilerParams(collective_id=0, has_side_effects=True, vmem_limit_bytes=66_500_000),
        cost_estimate=pl.CostEstimate(flops=16 * num_loc * slots * model * width,
                                      bytes_accessed=70 * 2 ** 20, transcendentals=0),
        name='stage_layer',
    )(ids, gates, x_acts, d_out, w_in, w_up, w_out)


def weight_kernel(tall, wide, din_ref, dup_ref, dout_ref):
    for e in range(tall.shape[0]):
        din_ref[e] = dot(tall[e, 0], wide[e, 0, 0]).astype(BF16)
        dup_ref[e] = dot(tall[e, 0], wide[e, 0, 1]).astype(BF16)
        dout_ref[e] = dot(tall[e, 1], wide[e, 0, 2]).T.astype(BF16)


def weight_call(wide, tall):
    num_loc, tiles, _, slots, _ = wide.shape
    model, width = tall.shape[2], tiles * TILE
    return pl.pallas_call(
        weight_kernel,
        grid=(tiles,),
        in_specs=[pl.BlockSpec(tall.shape, lambda t: (0, 0, 0, 0)),
                  pl.BlockSpec((num_loc, 1, 3, slots, TILE), lambda t: (0, t, 0, 0, 0))],
        out_specs=[pl.BlockSpec((num_loc, model, TILE), lambda t: (0, 0, t))] * 2
        + [pl.BlockSpec((num_loc, TILE, model), lambda t: (0, t, 0))],
        out_shape=[jax.ShapeDtypeStruct((num_loc, model, width), BF16)] * 2
        + [jax.ShapeDtypeStruct((num_loc, width, model), BF16)],
        compiler_params=pltpu.CompilerParams(dimension_semantics=('arbitrary',)),
        cost_estimate=pl.CostEstimate(flops=6 * num_loc * slots * model * width,
                                      bytes_accessed=50 * 2 ** 20, transcendentals=0),
        name='weight_grads',
    )(tall, wide)


def solution(mesh):
    group = mesh.shape['expert']
    stages = mesh.shape['stage']

    def device_fn(x_acts, expert_ids, gate_wts, w_in, w_up, w_out, d_out):
        num_loc = w_in.shape[1]
        tokens = x_acts.shape[2]
        top_k = expert_ids.shape[3]
        cap = 3 * top_k * tokens // (2 * num_loc * group)
        ids = jnp.swapaxes(expert_ids[:, 0], 1, 2)
        gates = jnp.swapaxes(gate_wts[:, 0], 1, 2)
        dx_home, y_loc, y_x, wide, tall = stage_call(
            stages, cap, ids, gates, x_acts, d_out, w_in, w_up, w_out)
        d_x = lax.ppermute(dx_home, 'stage', [((s + 1) % stages, s) for s in range(stages)])
        y_in = lax.ppermute(y_x, 'expert', [(i, i ^ 2) for i in range(group)])
        d_in, d_up, d_wout = weight_call(wide, tall)
        y = (y_loc.astype(F32) + y_in.astype(F32)).astype(BF16)
        return y[None], d_x[None], d_in[None], d_up[None], d_wout[None]

    tok_spec = P(None, 'stage', 'expert', None)
    w_spec = P('stage', 'expert', None, None)
    row_spec = P('stage', 'expert', None)
    return jax.shard_map(device_fn, mesh=mesh,
                         in_specs=(tok_spec, tok_spec, tok_spec, w_spec, w_spec, w_spec, row_spec),
                         out_specs=(row_spec, row_spec, w_spec, w_spec, w_spec), check_vma=False)
```

```python
import functools

import jax
import jax.numpy as jnp
from jax import lax
from jax.experimental import pallas as pl
from jax.experimental.pallas import tpu as pltpu
from jax.sharding import PartitionSpec as P

BF16 = jnp.bfloat16
F32 = jnp.float32
MESH = pl.DeviceIdType.MESH
TILE = 256
PARTS = 4
EARLY = 2
A, B, A_FAR, B_FAR = range(4)


def dot(lhs, rhs, lc=1, rc=0):
    return lax.dot_general(lhs, rhs, (((lc,), (rc,)), ((), ())), preferred_element_type=F32)


def routing(mb, num_loc, ids, gates, pos, gate_rows, pos_cols):
    first = lax.axis_index('expert') * num_loc
    tokens = ids.shape[-1]
    rows = 4 * num_loc
    lane = lax.broadcasted_iota(jnp.int32, (rows, tokens), 1)
    sub = lax.broadcasted_iota(jnp.int32, (rows, tokens), 0)
    expert = first + sub % num_loc

    def field(ref, k):
        return jnp.concatenate([ref[s, mb, k:k + 1, :] for s in range(4) for _ in range(num_loc)], axis=0)

    hit0, hit1 = field(ids, 0) == expert, field(ids, 1) == expert
    gate_rows[mb] = jnp.where(hit0, field(gates, 0), 0.0) + jnp.where(hit1, field(gates, 1), 0.0)
    taken = jnp.where(hit0 | hit1, 1, 0)
    run = taken
    step = 1
    while step < tokens:
        run = run + jnp.where(lane >= step, pltpu.roll(run, step, 1), 0)
        step *= 2
    slot = jnp.where(taken == 1, run - 1, -1)
    pos[mb] = slot
    pos_cols[mb, :, 0:rows] = slot.T


def pick(pos, gate_rows, mb, row, cap):
    tokens = pos.shape[-1]
    hit = pos[mb, pl.ds(row, 1), :] == lax.broadcasted_iota(jnp.int32, (cap, tokens), 0)
    gate = jnp.sum(jnp.where(hit, gate_rows[mb, pl.ds(row, 1), :], 0.0), axis=1, keepdims=True)
    return jnp.where(hit, 1.0, 0.0).astype(BF16), gate


def to_tokens(pos_cols, mb, block, rows, out):
    num_loc, cap, _ = rows.shape
    part = out.shape[2] // PARTS
    for m in range(PARTS):
        span = slice(m * part, (m + 1) * part)
        cols = pltpu.roll(pos_cols[mb, span, :], lax.rem(128 - num_loc * block, 128), 1)
        slot = lax.broadcasted_iota(jnp.int32, (part, cap), 1)
        sel = [jnp.where(cols[:, e:e + 1] == slot, 1.0, 0.0).astype(BF16) for e in range(num_loc)]
        total = dot(jnp.concatenate(sel, axis=1), rows[...].reshape(num_loc * cap, rows.shape[2]))
        out[mb, block, span, :] = total.astype(BF16)


def add_bf16(*refs):
    total = refs[0][...].astype(F32)
    for ref in refs[1:]:
        total += ref[...].astype(F32)
    return total.astype(BF16)


def stage_kernel(num_stages, cap, ids_in, gates_in, x_hbm, dy_hbm, win_hbm, wup_hbm, wout_hbm,
                 dx_hbm, y_hbm, yx_hbm, wide_hbm, tall_hbm,
                 ids, gates, xs, dys, win, wup, wout, pos, gate_rows, pos_cols, rows, ret, rin, cin,
                 wide_buf, tall_buf, q_early, u_early,
                 meta_send, meta_recv, hop_send, hop_recv, fwd_send, fwd_recv, dy_sem, dy_send, dy_recv,
                 ret_send, ret_recv, crs_send, crs_recv, w_sem, out_sem, res_sem, pace):
    stage, me = lax.axis_index('stage'), lax.axis_index('expert')
    nxt, prv = lax.rem(stage + 1, num_stages), lax.rem(stage + num_stages - 1, num_stages)
    core, chip = lax.rem(me, 2), me // 2
    other = 1 - core

    def peer(flip):
        new_core = other if flip % 2 else core
        new_chip = 1 - chip if flip // 2 else chip
        return 2 * new_chip + new_core

    partner, across = (stage, peer(1)), (stage, peer(2))
    num_loc, model, width = win.shape
    tokens = xs.shape[2]
    part = tokens // PARTS
    tiles = width // TILE

    def remote(src, dst, send, recv, device):
        return pltpu.make_async_remote_copy(src_ref=src, dst_ref=dst, send_sem=send, recv_sem=recv,
                                            device_id=device, device_id_type=MESH)

    def meta(flip, k, block=None):
        src, dst = ((ids_in, ids), (gates_in, gates))[k]
        block = 2 * (flip // 2) + core if block is None else block
        return remote(src, dst.at[block], meta_send.at[k, flip], meta_recv.at[k, block], (nxt, peer(flip)))

    def piece(mb, block, k):
        return xs.at[mb, block, pl.ds(k * part, part)]

    def hop(mb, k):
        src = x_hbm.at[mb, 0, pl.ds(k * part, part)]
        return remote(src, piece(mb, core, k), hop_send.at[mb, k], hop_recv.at[mb, k], (nxt, me))

    def near(mb, k, block=None):
        ref = piece(mb, core if block is None else block, k)
        return remote(ref, ref, fwd_send.at[mb, 0, k], fwd_recv.at[mb, 0, k], partner)

    def cross(mb, k):
        return remote(piece(mb, core, k), piece(mb, 2 + core, k), fwd_send.at[mb, 1, k], fwd_recv.at[mb, 1, k],
                      across)

    def far(mb, k, block=None):
        ref = piece(mb, 2 + core if block is None else block, k)
        return remote(ref, ref, fwd_send.at[mb, 2, k], fwd_recv.at[mb, 2, k], partner)

    def near_arrived(mb):
        for k in range(PARTS):
            near(mb, k, other).wait_recv()

    def far_arrived(mb):
        for k in range(PARTS):
            far(mb, k, 2 + other).wait_recv()

    dy_own = pltpu.make_async_copy(dy_hbm.at[0], dys.at[core], dy_sem)
    dy_near = remote(dy_hbm.at[0], dys.at[core], dy_send.at[0], dy_recv.at[0], partner)
    dy_near_in = remote(dy_hbm.at[0], dys.at[other], dy_send.at[0], dy_recv.at[0], partner)
    dy_cross = remote(dy_hbm.at[0], dys.at[2 + core], dy_send.at[1], dy_recv.at[1], across)
    dy_far = remote(dys.at[2 + core], dys.at[2 + core], dy_send.at[2], dy_recv.at[2], partner)
    dy_far_in = remote(dys.at[2 + other], dys.at[2 + other], dy_send.at[2], dy_recv.at[2], partner)

    def back(mb, k, block=None):
        src = ret.at[mb, 2 * k + other if block is None else block]
        return remote(src, rin.at[mb, k], ret_send.at[mb, k], ret_recv.at[mb, k], partner)

    def send_back(mb, block):
        @pl.when(lax.rem(block, 2) != core)
        def _():
            back(mb, block // 2, block).start()

    dx_cross = remote(ret.at[0, 2 + core], cin, crs_send, crs_recv, across)

    def dx_across():
        back(0, 1).wait_recv()
        ret[0, 2 + core] = add_bf16(ret.at[0, 2 + core], rin.at[0, 1])
        dx_cross.start()

    dx_save = pltpu.make_async_copy(ret.at[0, core], dx_hbm, res_sem.at[0])
    y_save = pltpu.make_async_copy(ret.at[1, core], y_hbm, res_sem.at[1])
    yx_save = pltpu.make_async_copy(ret.at[1, 2 + core], yx_hbm, res_sem.at[2])

    weights = [pltpu.make_async_copy(src.at[0], dst, w_sem.at[k])
               for k, (src, dst) in enumerate(((win_hbm, win), (wup_hbm, wup), (wout_hbm, wout)))]

    def outs(st):
        slot = lax.rem(st, 2)
        block, e = st // num_loc, lax.rem(st, num_loc)
        span = pl.ds(pl.multiple_of(block * cap, cap), cap)
        return (pltpu.make_async_copy(wide_buf.at[slot], wide_hbm.at[e, :, :, span], out_sem.at[slot, 0]),
                pltpu.make_async_copy(tall_buf.at[slot], tall_hbm.at[e, :, :, span], out_sem.at[slot, 1]))

    def at(now, when, on_core=None):
        cond = now == when if on_core is None else (now == when) & (core == on_core)
        return pl.when(cond)

    barrier = pltpu.get_barrier_semaphore()
    for device in [(prv, peer(flip)) for flip in range(4)] + [partner, across]:
        pl.semaphore_signal(barrier, inc=1, device_id=device, device_id_type=MESH)
    pl.semaphore_wait(barrier, 6)

    for flip in range(4):
        for k in range(2):
            meta(flip, k).start()

    @pl.when(core == 0)
    def _():
        for k in range(PARTS):
            hop(0, k).start()
        dy_cross.start()

    dy_near.start()
    dy_own.start()
    for copy in weights:
        copy.start()

    for block in range(4):
        for k in range(2):
            meta(0, k, block).wait_recv()
    for mb in range(2):
        routing(mb, num_loc, ids, gates, pos, gate_rows, pos_cols)
    dy_own.wait()
    dy_near_in.wait_recv()
    for copy in weights:
        copy.wait()

    def cotangent(st):
        sel, gate = pick(pos, gate_rows, 0, st, cap)
        return sel, gate * dot(sel, dys[st // num_loc])

    def early_step(st, carry):
        q = cotangent(st)[1].astype(BF16)
        q_early[st] = q
        for t in range(tiles):
            cols = slice(t * TILE, (t + 1) * TILE)
            u_early[st, :, cols] = dot(q, wout[lax.rem(st, num_loc), cols, :], 1, 1)
        return carry

    lax.fori_loop(0, EARLY, early_step, 0)

    @pl.when(core == 0)
    def _():
        for k in range(PARTS):
            hop(0, k).wait_recv()
            near(0, k).start()
            cross(0, k).start()
            if k == PARTS - 2:
                pl.semaphore_signal(pace, inc=1, device_id=partner, device_id_type=MESH)

    @pl.when(core == 1)
    def _():
        pl.semaphore_wait(pace, 1)
        for k in range(PARTS):
            hop(0, k).start()
        dy_cross.start()
        near_arrived(0)

    steps = 4 * num_loc
    half, most = PARTS // 2, PARTS - 1

    def pass_on(mb, lo, hi):
        for k in range(lo, hi):
            hop(mb, k).wait_recv()
            near(mb, k).start()
            cross(mb, k).start()

    def pass_far(mb, lo, hi):
        for k in range(lo, hi):
            cross(mb, k).wait_recv()
            far(mb, k).start()

    def backward_step(early, st, carry):
        block, e = st // num_loc, lax.rem(st, num_loc)
        slot = lax.rem(st, 2)

        @at(st, 1, on_core=1)
        def _():
            pass_on(0, 0, most)

        @at(st, num_loc, on_core=1)
        def _():
            pass_on(0, most, PARTS)

        @at(st, num_loc, on_core=0)
        def _():
            for k in range(PARTS):
                hop(1, k).start()
            near_arrived(0)

        @at(st, num_loc + 1, on_core=0)
        def _():
            dy_cross.wait_recv()
            dy_far.start()
            pass_far(0, 0, PARTS)

        @at(st, 2 * num_loc, on_core=0)
        def _():
            pass_on(1, 0, half)

        @at(st, 2 * num_loc, on_core=1)
        def _():
            for k in range(PARTS):
                hop(1, k).start()
            far_arrived(0)
            dy_far_in.wait_recv()

        @at(st, 2 * num_loc + 1, on_core=0)
        def _():
            pass_on(1, half, PARTS)

        @at(st, 2 * num_loc + 1, on_core=1)
        def _():
            dy_cross.wait_recv()
            dy_far.start()
            pass_far(0, 0, most)

        @at(st, 3 * num_loc, on_core=1)
        def _():
            pass_far(0, most, PARTS)
            pass_on(1, 0, half)

        @at(st, 3 * num_loc, on_core=0)
        def _():
            far_arrived(0)
            dy_far_in.wait_recv()

        @at(st, 3 * num_loc + 1, on_core=1)
        def _():
            pass_on(1, half, PARTS)

        @at(st, 3 * num_loc + 1, on_core=0)
        def _():
            dx_across()

        @pl.when(st >= 2)
        def _():
            for copy in outs(st - 2):
                copy.wait()

        if early:
            sel = pick(pos, gate_rows, 0, st, cap)[0]
            gdy = q_early[st].astype(F32)
        else:
            sel, gdy = cotangent(st)
        x = dot(sel, xs[0, block])
        tall_buf[slot, 0] = x.T.astype(BF16)
        tall_buf[slot, 1] = gdy.T.astype(BF16)
        x, q = x.astype(BF16), gdy.astype(BF16)
        for t in range(tiles):
            cols = slice(t * TILE, (t + 1) * TILE)
            a = dot(x, win[e, :, cols])
            b = dot(x, wup[e, :, cols])
            u = u_early[st, :, cols] if early else dot(q, wout[e, cols, :], 1, 1)
            sig = jax.nn.sigmoid(a)
            act = a * sig
            wide_buf[slot, t, 0] = (u * b * sig * (1.0 + a * (1.0 - sig))).astype(BF16)
            wide_buf[slot, t, 1] = (u * act).astype(BF16)
            wide_buf[slot, t, 2] = (act * b).astype(BF16)
        g_in = jnp.concatenate([wide_buf[slot, t, 0] for t in range(tiles)], axis=1)
        g_up = jnp.concatenate([wide_buf[slot, t, 1] for t in range(tiles)], axis=1)
        rows[e] = (dot(g_in, win[e], 1, 1) + dot(g_up, wup[e], 1, 1)).astype(BF16)
        for copy in outs(st):
            copy.start()

        @pl.when(e == num_loc - 1)
        def _():
            to_tokens(pos_cols, 0, block, rows, ret)
            send_back(0, block)

        return carry

    lax.fori_loop(0, EARLY, functools.partial(backward_step, True), 0)
    lax.fori_loop(EARLY, steps, functools.partial(backward_step, False), 0)
    for st in (steps - 2, steps - 1):
        for copy in outs(st):
            copy.wait()

    def forward_step(st, carry):
        block, e = st // num_loc, lax.rem(st, num_loc)

        @at(st, 0, on_core=1)
        def _():
            near_arrived(1)

        @at(st, 1, on_core=1)
        def _():
            dx_across()

        @at(st, num_loc, on_core=0)
        def _():
            near_arrived(1)

        @at(st, num_loc + 1, on_core=0)
        def _():
            pass_far(1, 0, PARTS)

        @at(st, 2 * num_loc, on_core=1)
        def _():
            far_arrived(1)

        @at(st, 2 * num_loc + 1, on_core=1)
        def _():
            pass_far(1, 0, most)

        @at(st, 3 * num_loc, on_core=1)
        def _():
            pass_far(1, most, PARTS)

        @at(st, 3 * num_loc)
        def _():
            back(1, 0).wait_recv()
            ret[1, core] = add_bf16(ret.at[1, core], rin.at[1, 0])
            y_save.start()

        @at(st, 3 * num_loc, on_core=0)
        def _():
            far_arrived(1)

        sel, gate = pick(pos, gate_rows, 1, st, cap)
        x = dot(sel, xs[1, block]).astype(BF16)
        for t in range(tiles):
            cols = slice(t * TILE, (t + 1) * TILE)
            a = dot(x, win[e, :, cols])
            b = dot(x, wup[e, :, cols])
            wide_buf[0, t, 0] = (a * jax.nn.sigmoid(a) * b).astype(BF16)
        hid = jnp.concatenate([wide_buf[0, t, 0] for t in range(tiles)], axis=1)
        rows[e] = (gate * dot(hid, wout[e])).astype(BF16)

        @pl.when(e == num_loc - 1)
        def _():
            to_tokens(pos_cols, 1, block, rows, ret)
            send_back(1, block)

        return carry

    lax.fori_loop(0, steps, forward_step, 0)
    back(1, 1).wait_recv()
    ret[1, 2 + core] = add_bf16(ret.at[1, 2 + core], rin.at[1, 1])
    yx_save.start()
    back(0, 0).wait_recv()
    dx_cross.wait_recv()
    ret[0, core] = add_bf16(ret.at[0, core], rin.at[0, 0], cin)
    dx_save.start()

    for flip in range(4):
        for k in range(2):
            meta(flip, k).wait_send()
    for mb in range(2):
        for k in range(PARTS):
            hop(mb, k).wait_send()
            near(mb, k).wait_send()
            cross(mb, k).wait_send()
            far(mb, k).wait_send()
        for k in range(2):
            back(mb, k).wait_send()
    for copy in (dy_near, dy_cross, dy_far, dx_cross):
        copy.wait_send()
    for copy in (y_save, yx_save, dx_save):
        copy.wait()


def stage_call(num_stages, cap, ids, gates, x_acts, d_out, w_in, w_up, w_out):
    _, num_loc, model, width = w_in.shape
    tokens = x_acts.shape[2]
    slots = 4 * cap
    whole = pl.BlockSpec(memory_space=pltpu.VMEM)
    anyspace = pl.BlockSpec(memory_space=pl.ANY)
    block = jax.ShapeDtypeStruct((tokens, model), BF16)
    wide = jax.ShapeDtypeStruct((num_loc, width // TILE, 3, slots, TILE), BF16)
    tall = jax.ShapeDtypeStruct((num_loc, 2, model, slots), BF16)
    vmem = pltpu.VMEM
    dma = pltpu.SemaphoreType.DMA
    return pl.pallas_call(
        functools.partial(stage_kernel, num_stages, cap),
        out_shape=[block] * 3 + [wide, tall],
        in_specs=[whole] * 2 + [anyspace] * 5,
        out_specs=[anyspace] * 5,
        scratch_shapes=[
            vmem((4,) + ids.shape, jnp.int32), vmem((4,) + gates.shape, F32),
            vmem((2, 4, tokens, model), BF16), vmem((4, tokens, model), BF16),
            vmem((num_loc, model, width), BF16), vmem((num_loc, model, width), BF16),
            vmem((num_loc, width, model), BF16),
            vmem((2, 4 * num_loc, tokens), jnp.int32), vmem((2, 4 * num_loc, tokens), F32),
            vmem((2, tokens, 128), jnp.int32),
            vmem((num_loc, cap, model), BF16), vmem((2, 4, tokens, model), BF16),
            vmem((2, 2, tokens, model), BF16), vmem((tokens, model), BF16),
            vmem((2, width // TILE, 3, cap, TILE), BF16), vmem((2, 2, model, cap), BF16),
            vmem((EARLY, cap, model), BF16), vmem((EARLY, cap, width), F32),
            dma((2, 4)), dma((2, 4)), dma((2, PARTS)), dma((2, PARTS)), dma((2, 3, PARTS)), dma((2, 3, PARTS)),
            dma, dma((3,)), dma((3,)), dma((2, 2)), dma((2, 2)), dma, dma, dma((3,)), dma((2, 2)), dma((3,)),
            pltpu.SemaphoreType.REGULAR,
        ],
        compiler_params=pltpu.CompilerParams(collective_id=0, has_side_effects=True, vmem_limit_bytes=66_500_000),
        cost_estimate=pl.CostEstimate(flops=16 * num_loc * slots * model * width,
                                      bytes_accessed=70 * 2 ** 20, transcendentals=0),
        name='stage_layer',
    )(ids, gates, x_acts, d_out, w_in, w_up, w_out)


def weight_kernel(tall, wide, din_ref, dup_ref, dout_ref):
    for e in range(tall.shape[0]):
        din_ref[e] = dot(tall[e, 0], wide[e, 0, 0]).astype(BF16)
        dup_ref[e] = dot(tall[e, 0], wide[e, 0, 1]).astype(BF16)
        dout_ref[e] = dot(tall[e, 1], wide[e, 0, 2]).T.astype(BF16)


def weight_call(wide, tall):
    num_loc, tiles, _, slots, _ = wide.shape
    model, width = tall.shape[2], tiles * TILE
    return pl.pallas_call(
        weight_kernel,
        grid=(tiles,),
        in_specs=[pl.BlockSpec(tall.shape, lambda t: (0, 0, 0, 0)),
                  pl.BlockSpec((num_loc, 1, 3, slots, TILE), lambda t: (0, t, 0, 0, 0))],
        out_specs=[pl.BlockSpec((num_loc, model, TILE), lambda t: (0, 0, t))] * 2
        + [pl.BlockSpec((num_loc, TILE, model), lambda t: (0, t, 0))],
        out_shape=[jax.ShapeDtypeStruct((num_loc, model, width), BF16)] * 2
        + [jax.ShapeDtypeStruct((num_loc, width, model), BF16)],
        compiler_params=pltpu.CompilerParams(dimension_semantics=('arbitrary',)),
        cost_estimate=pl.CostEstimate(flops=6 * num_loc * slots * model * width,
                                      bytes_accessed=50 * 2 ** 20, transcendentals=0),
        name='weight_grads',
    )(tall, wide)


def solution(mesh):
    group = mesh.shape['expert']
    stages = mesh.shape['stage']

    def device_fn(x_acts, expert_ids, gate_wts, w_in, w_up, w_out, d_out):
        num_loc = w_in.shape[1]
        tokens = x_acts.shape[2]
        top_k = expert_ids.shape[3]
        cap = 3 * top_k * tokens // (2 * num_loc * group)
        ids = jnp.swapaxes(expert_ids[:, 0], 1, 2)
        gates = jnp.swapaxes(gate_wts[:, 0], 1, 2)
        dx_home, y_loc, y_x, wide, tall = stage_call(
            stages, cap, ids, gates, x_acts, d_out, w_in, w_up, w_out)
        d_x = lax.ppermute(dx_home, 'stage', [((s + 1) % stages, s) for s in range(stages)])
        y_in = lax.ppermute(y_x, 'expert', [(i, i ^ 2) for i in range(group)])
        d_in, d_up, d_wout = weight_call(wide, tall)
        y = (y_loc.astype(F32) + y_in.astype(F32)).astype(BF16)
        return y[None], d_x[None], d_in[None], d_up[None], d_wout[None]

    tok_spec = P(None, 'stage', 'expert', None)
    w_spec = P('stage', 'expert', None, None)
    row_spec = P('stage', 'expert', None)
    return jax.shard_map(device_fn, mesh=mesh,
                         in_specs=(tok_spec, tok_spec, tok_spec, w_spec, w_spec, w_spec, row_spec),
                         out_specs=(row_spec, row_spec, w_spec, w_spec, w_spec), check_vma=False)
```

```python
import functools

import jax
import jax.numpy as jnp
from jax import lax
from jax.experimental import pallas as pl
from jax.experimental.pallas import tpu as pltpu
from jax.sharding import PartitionSpec as P

BF16 = jnp.bfloat16
F32 = jnp.float32
MESH = pl.DeviceIdType.MESH
TILE = 256
PARTS = 4
EARLY = 2
A, B, A_FAR, B_FAR = range(4)


def dot(lhs, rhs, lc=1, rc=0):
    return lax.dot_general(lhs, rhs, (((lc,), (rc,)), ((), ())), preferred_element_type=F32)


def routing(mb, num_loc, ids, gates, pos, gate_rows, pos_cols):
    first = lax.axis_index('expert') * num_loc
    tokens = ids.shape[-1]
    rows = 4 * num_loc
    lane = lax.broadcasted_iota(jnp.int32, (rows, tokens), 1)
    sub = lax.broadcasted_iota(jnp.int32, (rows, tokens), 0)
    expert = first + sub % num_loc

    def field(ref, k):
        return jnp.concatenate([ref[s, mb, k:k + 1, :] for s in range(4) for _ in range(num_loc)], axis=0)

    hit0, hit1 = field(ids, 0) == expert, field(ids, 1) == expert
    gate_rows[mb] = jnp.where(hit0, field(gates, 0), 0.0) + jnp.where(hit1, field(gates, 1), 0.0)
    taken = jnp.where(hit0 | hit1, 1, 0)
    run = taken
    step = 1
    while step < tokens:
        run = run + jnp.where(lane >= step, pltpu.roll(run, step, 1), 0)
        step *= 2
    slot = jnp.where(taken == 1, run - 1, -1)
    pos[mb] = slot
    pos_cols[mb, :, 0:rows] = slot.T


def pick(pos, gate_rows, mb, row, cap):
    tokens = pos.shape[-1]
    hit = pos[mb, pl.ds(row, 1), :] == lax.broadcasted_iota(jnp.int32, (cap, tokens), 0)
    gate = jnp.sum(jnp.where(hit, gate_rows[mb, pl.ds(row, 1), :], 0.0), axis=1, keepdims=True)
    return jnp.where(hit, 1.0, 0.0).astype(BF16), gate


def to_tokens(pos_cols, mb, block, rows, out):
    num_loc, cap, _ = rows.shape
    part = out.shape[2] // PARTS
    for m in range(PARTS):
        span = slice(m * part, (m + 1) * part)
        cols = pltpu.roll(pos_cols[mb, span, :], lax.rem(128 - num_loc * block, 128), 1)
        slot = lax.broadcasted_iota(jnp.int32, (part, cap), 1)
        sel = [jnp.where(cols[:, e:e + 1] == slot, 1.0, 0.0).astype(BF16) for e in range(num_loc)]
        total = dot(jnp.concatenate(sel, axis=1), rows[...].reshape(num_loc * cap, rows.shape[2]))
        out[mb, block, span, :] = total.astype(BF16)


def add_bf16(*refs):
    total = refs[0][...].astype(F32)
    for ref in refs[1:]:
        total += ref[...].astype(F32)
    return total.astype(BF16)


def stage_kernel(num_stages, cap, ids_in, gates_in, x_hbm, dy_hbm, win_hbm, wup_hbm, wout_hbm,
                 dx_hbm, y_hbm, yx_hbm, wide_hbm, tall_hbm,
                 ids, gates, xs, dys, win, wup, wout, pos, gate_rows, pos_cols, rows, ret, rin, cin,
                 wide_buf, tall_buf, q_early, u_early,
                 meta_send, meta_recv, hop_send, hop_recv, fwd_send, fwd_recv, dy_sem, dy_send, dy_recv,
                 ret_send, ret_recv, crs_send, crs_recv, w_sem, out_sem, res_sem, pace):
    stage, me = lax.axis_index('stage'), lax.axis_index('expert')
    nxt, prv = lax.rem(stage + 1, num_stages), lax.rem(stage + num_stages - 1, num_stages)
    core, chip = lax.rem(me, 2), me // 2
    other = 1 - core

    def peer(flip):
        new_core = other if flip % 2 else core
        new_chip = 1 - chip if flip // 2 else chip
        return 2 * new_chip + new_core

    partner, across = (stage, peer(1)), (stage, peer(2))
    num_loc, model, width = win.shape
    tokens = xs.shape[2]
    part = tokens // PARTS
    tiles = width // TILE

    def remote(src, dst, send, recv, device):
        return pltpu.make_async_remote_copy(src_ref=src, dst_ref=dst, send_sem=send, recv_sem=recv,
                                            device_id=device, device_id_type=MESH)

    def meta(flip, k, block=None):
        src, dst = ((ids_in, ids), (gates_in, gates))[k]
        block = 2 * (flip // 2) + core if block is None else block
        return remote(src, dst.at[block], meta_send.at[k, flip], meta_recv.at[k, block], (nxt, peer(flip)))

    def piece(mb, block, k):
        return xs.at[mb, block, pl.ds(k * part, part)]

    def hop(mb, k):
        src = x_hbm.at[mb, 0, pl.ds(k * part, part)]
        return remote(src, piece(mb, core, k), hop_send.at[mb, k], hop_recv.at[mb, k], (nxt, me))

    def near(mb, k, block=None):
        ref = piece(mb, core if block is None else block, k)
        return remote(ref, ref, fwd_send.at[mb, 0, k], fwd_recv.at[mb, 0, k], partner)

    def cross(mb, k):
        return remote(piece(mb, core, k), piece(mb, 2 + core, k), fwd_send.at[mb, 1, k], fwd_recv.at[mb, 1, k],
                      across)

    def far(mb, k, block=None):
        ref = piece(mb, 2 + core if block is None else block, k)
        return remote(ref, ref, fwd_send.at[mb, 2, k], fwd_recv.at[mb, 2, k], partner)

    def near_arrived(mb):
        for k in range(PARTS):
            near(mb, k, other).wait_recv()

    def far_arrived(mb):
        for k in range(PARTS):
            far(mb, k, 2 + other).wait_recv()

    dy_own = pltpu.make_async_copy(dy_hbm.at[0], dys.at[core], dy_sem)
    dy_near = remote(dy_hbm.at[0], dys.at[core], dy_send.at[0], dy_recv.at[0], partner)
    dy_near_in = remote(dy_hbm.at[0], dys.at[other], dy_send.at[0], dy_recv.at[0], partner)
    dy_cross = remote(dy_hbm.at[0], dys.at[2 + core], dy_send.at[1], dy_recv.at[1], across)
    dy_far = remote(dys.at[2 + core], dys.at[2 + core], dy_send.at[2], dy_recv.at[2], partner)
    dy_far_in = remote(dys.at[2 + other], dys.at[2 + other], dy_send.at[2], dy_recv.at[2], partner)

    def back(mb, k, block=None):
        src = ret.at[mb, 2 * k + other if block is None else block]
        return remote(src, rin.at[mb, k], ret_send.at[mb, k], ret_recv.at[mb, k], partner)

    def send_back(mb, block):
        @pl.when(lax.rem(block, 2) != core)
        def _():
            back(mb, block // 2, block).start()

    dx_cross = remote(ret.at[0, 2 + core], cin, crs_send, crs_recv, across)

    def dx_across():
        back(0, 1).wait_recv()
        ret[0, 2 + core] = add_bf16(ret.at[0, 2 + core], rin.at[0, 1])
        dx_cross.start()

    dx_save = pltpu.make_async_copy(ret.at[0, core], dx_hbm, res_sem.at[0])
    y_save = pltpu.make_async_copy(ret.at[1, core], y_hbm, res_sem.at[1])
    yx_save = pltpu.make_async_copy(ret.at[1, 2 + core], yx_hbm, res_sem.at[2])

    weights = [pltpu.make_async_copy(src.at[0], dst, w_sem.at[k])
               for k, (src, dst) in enumerate(((win_hbm, win), (wup_hbm, wup), (wout_hbm, wout)))]

    def outs(st):
        slot = lax.rem(st, 2)
        block, e = st // num_loc, lax.rem(st, num_loc)
        span = pl.ds(pl.multiple_of(block * cap, cap), cap)
        return (pltpu.make_async_copy(wide_buf.at[slot], wide_hbm.at[e, :, :, span], out_sem.at[slot, 0]),
                pltpu.make_async_copy(tall_buf.at[slot], tall_hbm.at[e, :, :, span], out_sem.at[slot, 1]))

    def at(now, when, on_core=None):
        cond = now == when if on_core is None else (now == when) & (core == on_core)
        return pl.when(cond)

    barrier = pltpu.get_barrier_semaphore()
    for device in [(prv, peer(flip)) for flip in range(4)] + [partner, across]:
        pl.semaphore_signal(barrier, inc=1, device_id=device, device_id_type=MESH)
    pl.semaphore_wait(barrier, 6)

    for flip in range(4):
        for k in range(2):
            meta(flip, k).start()

    @pl.when(core == 0)
    def _():
        for k in range(PARTS):
            hop(0, k).start()
        dy_cross.start()

    dy_near.start()
    dy_own.start()
    for copy in weights:
        copy.start()

    for block in range(4):
        for k in range(2):
            meta(0, k, block).wait_recv()
    for mb in range(2):
        routing(mb, num_loc, ids, gates, pos, gate_rows, pos_cols)
    dy_own.wait()
    dy_near_in.wait_recv()
    for copy in weights:
        copy.wait()

    def cotangent(st):
        sel, gate = pick(pos, gate_rows, 0, st, cap)
        return sel, gate * dot(sel, dys[st // num_loc])

    def early_step(st, carry):
        q = cotangent(st)[1].astype(BF16)
        q_early[st] = q
        for t in range(tiles):
            cols = slice(t * TILE, (t + 1) * TILE)
            u_early[st, :, cols] = dot(q, wout[lax.rem(st, num_loc), cols, :], 1, 1)
        return carry

    lax.fori_loop(0, EARLY, early_step, 0)

    @pl.when(core == 0)
    def _():
        for k in range(PARTS):
            hop(0, k).wait_recv()
            near(0, k).start()
            cross(0, k).start()
            if k == PARTS - 2:
                pl.semaphore_signal(pace, inc=1, device_id=partner, device_id_type=MESH)

    @pl.when(core == 1)
    def _():
        pl.semaphore_wait(pace, 1)
        for k in range(PARTS):
            hop(0, k).start()
        near_arrived(0)

    steps = 4 * num_loc
    half, most = PARTS // 2, PARTS - 1

    def pass_on(mb, lo, hi):
        for k in range(lo, hi):
            hop(mb, k).wait_recv()
            near(mb, k).start()
            cross(mb, k).start()

    def pass_far(mb, lo, hi):
        for k in range(lo, hi):
            cross(mb, k).wait_recv()
            far(mb, k).start()

    def backward_step(early, st, carry):
        block, e = st // num_loc, lax.rem(st, num_loc)
        slot = lax.rem(st, 2)

        @at(st, 1, on_core=1)
        def _():
            dy_cross.start()
            pass_on(0, 0, most)

        @at(st, num_loc, on_core=1)
        def _():
            pass_on(0, most, PARTS)

        @at(st, num_loc, on_core=0)
        def _():
            for k in range(PARTS):
                hop(1, k).start()
            near_arrived(0)

        @at(st, num_loc + 1, on_core=0)
        def _():
            dy_cross.wait_recv()
            dy_far.start()
            pass_far(0, 0, PARTS)

        @at(st, 2 * num_loc, on_core=1)
        def _():
            for k in range(PARTS):
                hop(1, k).start()
            far_arrived(0)
            dy_far_in.wait_recv()

        @at(st, 2 * num_loc + 1, on_core=0)
        def _():
            pass_on(1, 0, PARTS)

        @at(st, 2 * num_loc + 1, on_core=1)
        def _():
            dy_cross.wait_recv()
            dy_far.start()
            pass_far(0, 0, half)

        @at(st, 3 * num_loc, on_core=1)
        def _():
            pass_far(0, half, PARTS)
            pass_on(1, 0, half)

        @at(st, 3 * num_loc, on_core=0)
        def _():
            far_arrived(0)
            dy_far_in.wait_recv()

        @at(st, 3 * num_loc + 1, on_core=1)
        def _():
            pass_on(1, half, PARTS)

        @at(st, 3 * num_loc + 1, on_core=0)
        def _():
            dx_across()

        @pl.when(st >= 2)
        def _():
            for copy in outs(st - 2):
                copy.wait()

        if early:
            sel = pick(pos, gate_rows, 0, st, cap)[0]
            gdy = q_early[st].astype(F32)
        else:
            sel, gdy = cotangent(st)
        x = dot(sel, xs[0, block])
        tall_buf[slot, 0] = x.T.astype(BF16)
        tall_buf[slot, 1] = gdy.T.astype(BF16)
        x, q = x.astype(BF16), gdy.astype(BF16)
        for t in range(tiles):
            cols = slice(t * TILE, (t + 1) * TILE)
            a = dot(x, win[e, :, cols])
            b = dot(x, wup[e, :, cols])
            u = u_early[st, :, cols] if early else dot(q, wout[e, cols, :], 1, 1)
            sig = jax.nn.sigmoid(a)
            act = a * sig
            wide_buf[slot, t, 0] = (u * b * sig * (1.0 + a * (1.0 - sig))).astype(BF16)
            wide_buf[slot, t, 1] = (u * act).astype(BF16)
            wide_buf[slot, t, 2] = (act * b).astype(BF16)
        g_in = jnp.concatenate([wide_buf[slot, t, 0] for t in range(tiles)], axis=1)
        g_up = jnp.concatenate([wide_buf[slot, t, 1] for t in range(tiles)], axis=1)
        rows[e] = (dot(g_in, win[e], 1, 1) + dot(g_up, wup[e], 1, 1)).astype(BF16)
        for copy in outs(st):
            copy.start()

        @pl.when(e == num_loc - 1)
        def _():
            to_tokens(pos_cols, 0, block, rows, ret)
            send_back(0, block)

        return carry

    lax.fori_loop(0, EARLY, functools.partial(backward_step, True), 0)
    lax.fori_loop(EARLY, steps, functools.partial(backward_step, False), 0)
    for st in (steps - 2, steps - 1):
        for copy in outs(st):
            copy.wait()

    def forward_step(st, carry):
        block, e = st // num_loc, lax.rem(st, num_loc)

        @at(st, 0, on_core=1)
        def _():
            near_arrived(1)

        @at(st, 1, on_core=1)
        def _():
            dx_across()

        @at(st, num_loc, on_core=0)
        def _():
            near_arrived(1)

        @at(st, num_loc + 1, on_core=0)
        def _():
            pass_far(1, 0, PARTS)

        @at(st, 2 * num_loc, on_core=1)
        def _():
            far_arrived(1)

        @at(st, 2 * num_loc + 1, on_core=1)
        def _():
            pass_far(1, 0, most)

        @at(st, 3 * num_loc, on_core=1)
        def _():
            pass_far(1, most, PARTS)

        @at(st, 3 * num_loc)
        def _():
            back(1, 0).wait_recv()
            ret[1, core] = add_bf16(ret.at[1, core], rin.at[1, 0])
            y_save.start()

        @at(st, 3 * num_loc, on_core=0)
        def _():
            far_arrived(1)

        sel, gate = pick(pos, gate_rows, 1, st, cap)
        x = dot(sel, xs[1, block]).astype(BF16)
        for t in range(tiles):
            cols = slice(t * TILE, (t + 1) * TILE)
            a = dot(x, win[e, :, cols])
            b = dot(x, wup[e, :, cols])
            wide_buf[0, t, 0] = (a * jax.nn.sigmoid(a) * b).astype(BF16)
        hid = jnp.concatenate([wide_buf[0, t, 0] for t in range(tiles)], axis=1)
        rows[e] = (gate * dot(hid, wout[e])).astype(BF16)

        @pl.when(e == num_loc - 1)
        def _():
            to_tokens(pos_cols, 1, block, rows, ret)
            send_back(1, block)

        return carry

    lax.fori_loop(0, steps, forward_step, 0)
    back(1, 1).wait_recv()
    ret[1, 2 + core] = add_bf16(ret.at[1, 2 + core], rin.at[1, 1])
    yx_save.start()
    back(0, 0).wait_recv()
    dx_cross.wait_recv()
    ret[0, core] = add_bf16(ret.at[0, core], rin.at[0, 0], cin)
    dx_save.start()

    for flip in range(4):
        for k in range(2):
            meta(flip, k).wait_send()
    for mb in range(2):
        for k in range(PARTS):
            hop(mb, k).wait_send()
            near(mb, k).wait_send()
            cross(mb, k).wait_send()
            far(mb, k).wait_send()
        for k in range(2):
            back(mb, k).wait_send()
    for copy in (dy_near, dy_cross, dy_far, dx_cross):
        copy.wait_send()
    for copy in (y_save, yx_save, dx_save):
        copy.wait()


def stage_call(num_stages, cap, ids, gates, x_acts, d_out, w_in, w_up, w_out):
    _, num_loc, model, width = w_in.shape
    tokens = x_acts.shape[2]
    slots = 4 * cap
    whole = pl.BlockSpec(memory_space=pltpu.VMEM)
    anyspace = pl.BlockSpec(memory_space=pl.ANY)
    block = jax.ShapeDtypeStruct((tokens, model), BF16)
    wide = jax.ShapeDtypeStruct((num_loc, width // TILE, 3, slots, TILE), BF16)
    tall = jax.ShapeDtypeStruct((num_loc, 2, model, slots), BF16)
    vmem = pltpu.VMEM
    dma = pltpu.SemaphoreType.DMA
    return pl.pallas_call(
        functools.partial(stage_kernel, num_stages, cap),
        out_shape=[block] * 3 + [wide, tall],
        in_specs=[whole] * 2 + [anyspace] * 5,
        out_specs=[anyspace] * 5,
        scratch_shapes=[
            vmem((4,) + ids.shape, jnp.int32), vmem((4,) + gates.shape, F32),
            vmem((2, 4, tokens, model), BF16), vmem((4, tokens, model), BF16),
            vmem((num_loc, model, width), BF16), vmem((num_loc, model, width), BF16),
            vmem((num_loc, width, model), BF16),
            vmem((2, 4 * num_loc, tokens), jnp.int32), vmem((2, 4 * num_loc, tokens), F32),
            vmem((2, tokens, 128), jnp.int32),
            vmem((num_loc, cap, model), BF16), vmem((2, 4, tokens, model), BF16),
            vmem((2, 2, tokens, model), BF16), vmem((tokens, model), BF16),
            vmem((2, width // TILE, 3, cap, TILE), BF16), vmem((2, 2, model, cap), BF16),
            vmem((EARLY, cap, model), BF16), vmem((EARLY, cap, width), F32),
            dma((2, 4)), dma((2, 4)), dma((2, PARTS)), dma((2, PARTS)), dma((2, 3, PARTS)), dma((2, 3, PARTS)),
            dma, dma((3,)), dma((3,)), dma((2, 2)), dma((2, 2)), dma, dma, dma((3,)), dma((2, 2)), dma((3,)),
            pltpu.SemaphoreType.REGULAR,
        ],
        compiler_params=pltpu.CompilerParams(collective_id=0, has_side_effects=True, vmem_limit_bytes=66_500_000),
        cost_estimate=pl.CostEstimate(flops=16 * num_loc * slots * model * width,
                                      bytes_accessed=70 * 2 ** 20, transcendentals=0),
        name='stage_layer',
    )(ids, gates, x_acts, d_out, w_in, w_up, w_out)


def weight_kernel(tall, wide, din_ref, dup_ref, dout_ref):
    for e in range(tall.shape[0]):
        din_ref[e] = dot(tall[e, 0], wide[e, 0, 0]).astype(BF16)
        dup_ref[e] = dot(tall[e, 0], wide[e, 0, 1]).astype(BF16)
        dout_ref[e] = dot(tall[e, 1], wide[e, 0, 2]).T.astype(BF16)


def weight_call(wide, tall):
    num_loc, tiles, _, slots, _ = wide.shape
    model, width = tall.shape[2], tiles * TILE
    return pl.pallas_call(
        weight_kernel,
        grid=(tiles,),
        in_specs=[pl.BlockSpec(tall.shape, lambda t: (0, 0, 0, 0)),
                  pl.BlockSpec((num_loc, 1, 3, slots, TILE), lambda t: (0, t, 0, 0, 0))],
        out_specs=[pl.BlockSpec((num_loc, model, TILE), lambda t: (0, 0, t))] * 2
        + [pl.BlockSpec((num_loc, TILE, model), lambda t: (0, t, 0))],
        out_shape=[jax.ShapeDtypeStruct((num_loc, model, width), BF16)] * 2
        + [jax.ShapeDtypeStruct((num_loc, width, model), BF16)],
        compiler_params=pltpu.CompilerParams(dimension_semantics=('arbitrary',)),
        cost_estimate=pl.CostEstimate(flops=6 * num_loc * slots * model * width,
                                      bytes_accessed=50 * 2 ** 20, transcendentals=0),
        name='weight_grads',
    )(tall, wide)


def solution(mesh):
    group = mesh.shape['expert']
    stages = mesh.shape['stage']

    def device_fn(x_acts, expert_ids, gate_wts, w_in, w_up, w_out, d_out):
        num_loc = w_in.shape[1]
        tokens = x_acts.shape[2]
        top_k = expert_ids.shape[3]
        cap = 3 * top_k * tokens // (2 * num_loc * group)
        ids = jnp.swapaxes(expert_ids[:, 0], 1, 2)
        gates = jnp.swapaxes(gate_wts[:, 0], 1, 2)
        dx_home, y_loc, y_x, wide, tall = stage_call(
            stages, cap, ids, gates, x_acts, d_out, w_in, w_up, w_out)
        d_x = lax.ppermute(dx_home, 'stage', [((s + 1) % stages, s) for s in range(stages)])
        y_in = lax.ppermute(y_x, 'expert', [(i, i ^ 2) for i in range(group)])
        d_in, d_up, d_wout = weight_call(wide, tall)
        y = (y_loc.astype(F32) + y_in.astype(F32)).astype(BF16)
        return y[None], d_x[None], d_in[None], d_up[None], d_wout[None]

    tok_spec = P(None, 'stage', 'expert', None)
    w_spec = P('stage', 'expert', None, None)
    row_spec = P('stage', 'expert', None)
    return jax.shard_map(device_fn, mesh=mesh,
                         in_specs=(tok_spec, tok_spec, tok_spec, w_spec, w_spec, w_spec, row_spec),
                         out_specs=(row_spec, row_spec, w_spec, w_spec, w_spec), check_vma=False)
```

```python
import functools

import jax
import jax.numpy as jnp
from jax import lax
from jax.experimental import pallas as pl
from jax.experimental.pallas import tpu as pltpu
from jax.sharding import PartitionSpec as P

BF16 = jnp.bfloat16
F32 = jnp.float32
MESH = pl.DeviceIdType.MESH
TILE = 256
PARTS = 4
A, B, A_FAR, B_FAR = range(4)


def dot(lhs, rhs, lc=1, rc=0):
    return lax.dot_general(lhs, rhs, (((lc,), (rc,)), ((), ())), preferred_element_type=F32)


def routing(mb, num_loc, ids, gates, pos, gate_rows, pos_cols):
    first = lax.axis_index('expert') * num_loc
    tokens = ids.shape[-1]
    rows = 4 * num_loc
    lane = lax.broadcasted_iota(jnp.int32, (rows, tokens), 1)
    sub = lax.broadcasted_iota(jnp.int32, (rows, tokens), 0)
    expert = first + sub % num_loc

    def field(ref, k):
        return jnp.concatenate([ref[s, mb, k:k + 1, :] for s in range(4) for _ in range(num_loc)], axis=0)

    hit0, hit1 = field(ids, 0) == expert, field(ids, 1) == expert
    gate_rows[mb] = jnp.where(hit0, field(gates, 0), 0.0) + jnp.where(hit1, field(gates, 1), 0.0)
    taken = jnp.where(hit0 | hit1, 1, 0)
    run = taken
    step = 1
    while step < tokens:
        run = run + jnp.where(lane >= step, pltpu.roll(run, step, 1), 0)
        step *= 2
    slot = jnp.where(taken == 1, run - 1, -1)
    pos[mb] = slot
    pos_cols[mb, :, 0:rows] = slot.T


def pick(pos, gate_rows, mb, row, cap):
    tokens = pos.shape[-1]
    hit = pos[mb, pl.ds(row, 1), :] == lax.broadcasted_iota(jnp.int32, (cap, tokens), 0)
    gate = jnp.sum(jnp.where(hit, gate_rows[mb, pl.ds(row, 1), :], 0.0), axis=1, keepdims=True)
    return jnp.where(hit, 1.0, 0.0).astype(BF16), gate


def to_tokens(pos_cols, mb, block, rows, out):
    num_loc, cap, _ = rows.shape
    part = out.shape[2] // PARTS
    for m in range(PARTS):
        span = slice(m * part, (m + 1) * part)
        cols = pltpu.roll(pos_cols[mb, span, :], lax.rem(128 - num_loc * block, 128), 1)
        slot = lax.broadcasted_iota(jnp.int32, (part, cap), 1)
        sel = [jnp.where(cols[:, e:e + 1] == slot, 1.0, 0.0).astype(BF16) for e in range(num_loc)]
        total = dot(jnp.concatenate(sel, axis=1), rows[...].reshape(num_loc * cap, rows.shape[2]))
        out[mb, block, span, :] = total.astype(BF16)


def add_bf16(*refs):
    total = refs[0][...].astype(F32)
    for ref in refs[1:]:
        total += ref[...].astype(F32)
    return total.astype(BF16)


def stage_kernel(num_stages, cap, ids_in, gates_in, x_hbm, dy_hbm, win_hbm, wup_hbm, wout_hbm,
                 dx_hbm, y_hbm, yx_hbm, wide_hbm, tall_hbm,
                 ids, gates, xs, dys, win, wup, wout, pos, gate_rows, pos_cols, rows, ret, rin, cin,
                 wide_buf, tall_buf,
                 meta_send, meta_recv, hop_send, hop_recv, fwd_send, fwd_recv, dy_sem, dy_send, dy_recv,
                 ret_send, ret_recv, crs_send, crs_recv, w_sem, out_sem, res_sem, pace):
    stage, me = lax.axis_index('stage'), lax.axis_index('expert')
    nxt, prv = lax.rem(stage + 1, num_stages), lax.rem(stage + num_stages - 1, num_stages)
    core, chip = lax.rem(me, 2), me // 2
    other = 1 - core

    def peer(flip):
        new_core = other if flip % 2 else core
        new_chip = 1 - chip if flip // 2 else chip
        return 2 * new_chip + new_core

    partner, across = (stage, peer(1)), (stage, peer(2))
    num_loc, model, width = win.shape
    tokens = xs.shape[2]
    part = tokens // PARTS
    tiles = width // TILE

    def remote(src, dst, send, recv, device):
        return pltpu.make_async_remote_copy(src_ref=src, dst_ref=dst, send_sem=send, recv_sem=recv,
                                            device_id=device, device_id_type=MESH)

    def meta(flip, k, block=None):
        src, dst = ((ids_in, ids), (gates_in, gates))[k]
        block = 2 * (flip // 2) + core if block is None else block
        return remote(src, dst.at[block], meta_send.at[k, flip], meta_recv.at[k, block], (nxt, peer(flip)))

    def piece(mb, block, k):
        return xs.at[mb, block, pl.ds(k * part, part)]

    def hop(mb, k):
        src = x_hbm.at[mb, 0, pl.ds(k * part, part)]
        return remote(src, piece(mb, core, k), hop_send.at[mb, k], hop_recv.at[mb, k], (nxt, me))

    def near(mb, k, block=None):
        ref = piece(mb, core if block is None else block, k)
        return remote(ref, ref, fwd_send.at[mb, 0, k], fwd_recv.at[mb, 0, k], partner)

    def cross(mb, k):
        return remote(piece(mb, core, k), piece(mb, 2 + core, k), fwd_send.at[mb, 1, k], fwd_recv.at[mb, 1, k],
                      across)

    def far(mb, k, block=None):
        ref = piece(mb, 2 + core if block is None else block, k)
        return remote(ref, ref, fwd_send.at[mb, 2, k], fwd_recv.at[mb, 2, k], partner)

    def near_arrived(mb):
        for k in range(PARTS):
            near(mb, k, other).wait_recv()

    def far_arrived(mb):
        for k in range(PARTS):
            far(mb, k, 2 + other).wait_recv()

    dy_own = pltpu.make_async_copy(dy_hbm.at[0], dys.at[core], dy_sem)
    dy_near = remote(dy_hbm.at[0], dys.at[core], dy_send.at[0], dy_recv.at[0], partner)
    dy_near_in = remote(dy_hbm.at[0], dys.at[other], dy_send.at[0], dy_recv.at[0], partner)
    dy_cross = remote(dy_hbm.at[0], dys.at[2 + core], dy_send.at[1], dy_recv.at[1], across)
    dy_far = remote(dys.at[2 + core], dys.at[2 + core], dy_send.at[2], dy_recv.at[2], partner)
    dy_far_in = remote(dys.at[2 + other], dys.at[2 + other], dy_send.at[2], dy_recv.at[2], partner)

    def back(mb, k, block=None):
        src = ret.at[mb, 2 * k + other if block is None else block]
        return remote(src, rin.at[mb, k], ret_send.at[mb, k], ret_recv.at[mb, k], partner)

    def send_back(mb, block):
        @pl.when(lax.rem(block, 2) != core)
        def _():
            back(mb, block // 2, block).start()

    dx_cross = remote(ret.at[0, 2 + core], cin, crs_send, crs_recv, across)

    def dx_across():
        back(0, 1).wait_recv()
        ret[0, 2 + core] = add_bf16(ret.at[0, 2 + core], rin.at[0, 1])
        dx_cross.start()

    dx_save = pltpu.make_async_copy(ret.at[0, core], dx_hbm, res_sem.at[0])
    y_save = pltpu.make_async_copy(ret.at[1, core], y_hbm, res_sem.at[1])
    yx_save = pltpu.make_async_copy(ret.at[1, 2 + core], yx_hbm, res_sem.at[2])

    weights = [pltpu.make_async_copy(src.at[0], dst, w_sem.at[k])
               for k, (src, dst) in enumerate(((win_hbm, win), (wup_hbm, wup), (wout_hbm, wout)))]

    def outs(st):
        slot = lax.rem(st, 2)
        block, e = st // num_loc, lax.rem(st, num_loc)
        span = pl.ds(pl.multiple_of(block * cap, cap), cap)
        return (pltpu.make_async_copy(wide_buf.at[slot], wide_hbm.at[e, :, :, span], out_sem.at[slot, 0]),
                pltpu.make_async_copy(tall_buf.at[slot], tall_hbm.at[e, :, :, span], out_sem.at[slot, 1]))

    def at(now, when, on_core=None):
        cond = now == when if on_core is None else (now == when) & (core == on_core)
        return pl.when(cond)

    barrier = pltpu.get_barrier_semaphore()
    for device in [(prv, peer(flip)) for flip in range(4)] + [partner, across]:
        pl.semaphore_signal(barrier, inc=1, device_id=device, device_id_type=MESH)
    pl.semaphore_wait(barrier, 6)

    for flip in range(4):
        for k in range(2):
            meta(flip, k).start()

    @pl.when(core == 0)
    def _():
        for k in range(PARTS):
            hop(0, k).start()
        dy_cross.start()

    dy_near.start()
    dy_own.start()
    for copy in weights:
        copy.start()

    for block in range(4):
        for k in range(2):
            meta(0, k, block).wait_recv()
    for mb in range(2):
        routing(mb, num_loc, ids, gates, pos, gate_rows, pos_cols)

    def cotangent(st):
        sel, gate = pick(pos, gate_rows, 0, st, cap)
        return sel, gate * dot(sel, dys[st // num_loc])

    @pl.when(core == 0)
    def _():
        for k in range(PARTS):
            hop(0, k).wait_recv()
            near(0, k).start()
            cross(0, k).start()
            if k == PARTS - 2:
                pl.semaphore_signal(pace, inc=1, device_id=partner, device_id_type=MESH)

    @pl.when(core == 1)
    def _():
        pl.semaphore_wait(pace, 1)
        for k in range(PARTS):
            hop(0, k).start()
        near_arrived(0)

    dy_own.wait()
    dy_near_in.wait_recv()
    for copy in weights:
        copy.wait()

    steps = 4 * num_loc
    half, most = PARTS // 2, PARTS - 1

    def pass_on(mb, lo, hi):
        for k in range(lo, hi):
            hop(mb, k).wait_recv()
            near(mb, k).start()
            cross(mb, k).start()

    def pass_far(mb, lo, hi):
        for k in range(lo, hi):
            cross(mb, k).wait_recv()
            far(mb, k).start()

    def backward_step(st, carry):
        block, e = st // num_loc, lax.rem(st, num_loc)
        slot = lax.rem(st, 2)

        @at(st, 1, on_core=1)
        def _():
            dy_cross.start()
            pass_on(0, 0, most)

        @at(st, num_loc, on_core=1)
        def _():
            pass_on(0, most, PARTS)

        @at(st, num_loc, on_core=0)
        def _():
            for k in range(PARTS):
                hop(1, k).start()
            near_arrived(0)

        @at(st, num_loc + 1, on_core=0)
        def _():
            dy_cross.wait_recv()
            dy_far.start()
            pass_far(0, 0, PARTS)

        @at(st, 2 * num_loc, on_core=1)
        def _():
            for k in range(PARTS):
                hop(1, k).start()
            far_arrived(0)
            dy_far_in.wait_recv()

        @at(st, 2 * num_loc + 1, on_core=0)
        def _():
            pass_on(1, 0, PARTS)

        @at(st, 2 * num_loc + 1, on_core=1)
        def _():
            dy_cross.wait_recv()
            dy_far.start()
            pass_far(0, 0, half)

        @at(st, 3 * num_loc, on_core=1)
        def _():
            pass_far(0, half, PARTS)
            pass_on(1, 0, half)

        @at(st, 3 * num_loc, on_core=0)
        def _():
            far_arrived(0)
            dy_far_in.wait_recv()

        @at(st, 3 * num_loc + 1, on_core=1)
        def _():
            pass_on(1, half, PARTS)

        @at(st, 3 * num_loc + 1, on_core=0)
        def _():
            dx_across()

        @pl.when(st >= 2)
        def _():
            for copy in outs(st - 2):
                copy.wait()

        sel, gdy = cotangent(st)
        x = dot(sel, xs[0, block])
        tall_buf[slot, 0] = x.T.astype(BF16)
        tall_buf[slot, 1] = gdy.T.astype(BF16)
        x, q = x.astype(BF16), gdy.astype(BF16)
        for t in range(tiles):
            cols = slice(t * TILE, (t + 1) * TILE)
            a = dot(x, win[e, :, cols])
            b = dot(x, wup[e, :, cols])
            u = dot(q, wout[e, cols, :], 1, 1)
            sig = jax.nn.sigmoid(a)
            act = a * sig
            wide_buf[slot, t, 0] = (u * b * sig * (1.0 + a * (1.0 - sig))).astype(BF16)
            wide_buf[slot, t, 1] = (u * act).astype(BF16)
            wide_buf[slot, t, 2] = (act * b).astype(BF16)
        g_in = jnp.concatenate([wide_buf[slot, t, 0] for t in range(tiles)], axis=1)
        g_up = jnp.concatenate([wide_buf[slot, t, 1] for t in range(tiles)], axis=1)
        rows[e] = (dot(g_in, win[e], 1, 1) + dot(g_up, wup[e], 1, 1)).astype(BF16)
        for copy in outs(st):
            copy.start()

        @pl.when(e == num_loc - 1)
        def _():
            to_tokens(pos_cols, 0, block, rows, ret)
            send_back(0, block)

        return carry

    lax.fori_loop(0, steps, backward_step, 0)
    for st in (steps - 2, steps - 1):
        for copy in outs(st):
            copy.wait()

    def forward_step(st, carry):
        block, e = st // num_loc, lax.rem(st, num_loc)

        @at(st, 0, on_core=1)
        def _():
            near_arrived(1)

        @at(st, 1, on_core=1)
        def _():
            dx_across()

        @at(st, num_loc, on_core=0)
        def _():
            near_arrived(1)

        @at(st, num_loc + 1, on_core=0)
        def _():
            pass_far(1, 0, PARTS)

        @at(st, 2 * num_loc, on_core=1)
        def _():
            far_arrived(1)

        @at(st, 2 * num_loc + 1, on_core=1)
        def _():
            pass_far(1, 0, most)

        @at(st, 3 * num_loc, on_core=1)
        def _():
            pass_far(1, most, PARTS)

        @at(st, 3 * num_loc)
        def _():
            back(1, 0).wait_recv()
            ret[1, core] = add_bf16(ret.at[1, core], rin.at[1, 0])
            y_save.start()

        @at(st, 3 * num_loc, on_core=0)
        def _():
            far_arrived(1)

        sel, gate = pick(pos, gate_rows, 1, st, cap)
        x = dot(sel, xs[1, block]).astype(BF16)
        for t in range(tiles):
            cols = slice(t * TILE, (t + 1) * TILE)
            a = dot(x, win[e, :, cols])
            b = dot(x, wup[e, :, cols])
            wide_buf[0, t, 0] = (a * jax.nn.sigmoid(a) * b).astype(BF16)
        hid = jnp.concatenate([wide_buf[0, t, 0] for t in range(tiles)], axis=1)
        rows[e] = (gate * dot(hid, wout[e])).astype(BF16)

        @pl.when(e == num_loc - 1)
        def _():
            to_tokens(pos_cols, 1, block, rows, ret)
            send_back(1, block)

        return carry

    lax.fori_loop(0, steps, forward_step, 0)
    back(1, 1).wait_recv()
    ret[1, 2 + core] = add_bf16(ret.at[1, 2 + core], rin.at[1, 1])
    yx_save.start()
    back(0, 0).wait_recv()
    dx_cross.wait_recv()
    ret[0, core] = add_bf16(ret.at[0, core], rin.at[0, 0], cin)
    dx_save.start()

    for flip in range(4):
        for k in range(2):
            meta(flip, k).wait_send()
    for mb in range(2):
        for k in range(PARTS):
            hop(mb, k).wait_send()
            near(mb, k).wait_send()
            cross(mb, k).wait_send()
            far(mb, k).wait_send()
        for k in range(2):
            back(mb, k).wait_send()
    for copy in (dy_near, dy_cross, dy_far, dx_cross):
        copy.wait_send()
    for copy in (y_save, yx_save, dx_save):
        copy.wait()


def stage_call(num_stages, cap, ids, gates, x_acts, d_out, w_in, w_up, w_out):
    _, num_loc, model, width = w_in.shape
    tokens = x_acts.shape[2]
    slots = 4 * cap
    whole = pl.BlockSpec(memory_space=pltpu.VMEM)
    anyspace = pl.BlockSpec(memory_space=pl.ANY)
    block = jax.ShapeDtypeStruct((tokens, model), BF16)
    wide = jax.ShapeDtypeStruct((num_loc, width // TILE, 3, slots, TILE), BF16)
    tall = jax.ShapeDtypeStruct((num_loc, 2, model, slots), BF16)
    vmem = pltpu.VMEM
    dma = pltpu.SemaphoreType.DMA
    return pl.pallas_call(
        functools.partial(stage_kernel, num_stages, cap),
        out_shape=[block] * 3 + [wide, tall],
        in_specs=[whole] * 2 + [anyspace] * 5,
        out_specs=[anyspace] * 5,
        scratch_shapes=[
            vmem((4,) + ids.shape, jnp.int32), vmem((4,) + gates.shape, F32),
            vmem((2, 4, tokens, model), BF16), vmem((4, tokens, model), BF16),
            vmem((num_loc, model, width), BF16), vmem((num_loc, model, width), BF16),
            vmem((num_loc, width, model), BF16),
            vmem((2, 4 * num_loc, tokens), jnp.int32), vmem((2, 4 * num_loc, tokens), F32),
            vmem((2, tokens, 128), jnp.int32),
            vmem((num_loc, cap, model), BF16), vmem((2, 4, tokens, model), BF16),
            vmem((2, 2, tokens, model), BF16), vmem((tokens, model), BF16),
            vmem((2, width // TILE, 3, cap, TILE), BF16), vmem((2, 2, model, cap), BF16),
            dma((2, 4)), dma((2, 4)), dma((2, PARTS)), dma((2, PARTS)), dma((2, 3, PARTS)), dma((2, 3, PARTS)),
            dma, dma((3,)), dma((3,)), dma((2, 2)), dma((2, 2)), dma, dma, dma((3,)), dma((2, 2)), dma((3,)),
            pltpu.SemaphoreType.REGULAR,
        ],
        compiler_params=pltpu.CompilerParams(collective_id=0, has_side_effects=True, vmem_limit_bytes=66_500_000),
        cost_estimate=pl.CostEstimate(flops=16 * num_loc * slots * model * width,
                                      bytes_accessed=70 * 2 ** 20, transcendentals=0),
        name='stage_layer',
    )(ids, gates, x_acts, d_out, w_in, w_up, w_out)


def weight_kernel(tall, wide, din_ref, dup_ref, dout_ref):
    for e in range(tall.shape[0]):
        din_ref[e] = dot(tall[e, 0], wide[e, 0, 0]).astype(BF16)
        dup_ref[e] = dot(tall[e, 0], wide[e, 0, 1]).astype(BF16)
        dout_ref[e] = dot(tall[e, 1], wide[e, 0, 2]).T.astype(BF16)


def weight_call(wide, tall):
    num_loc, tiles, _, slots, _ = wide.shape
    model, width = tall.shape[2], tiles * TILE
    return pl.pallas_call(
        weight_kernel,
        grid=(tiles,),
        in_specs=[pl.BlockSpec(tall.shape, lambda t: (0, 0, 0, 0)),
                  pl.BlockSpec((num_loc, 1, 3, slots, TILE), lambda t: (0, t, 0, 0, 0))],
        out_specs=[pl.BlockSpec((num_loc, model, TILE), lambda t: (0, 0, t))] * 2
        + [pl.BlockSpec((num_loc, TILE, model), lambda t: (0, t, 0))],
        out_shape=[jax.ShapeDtypeStruct((num_loc, model, width), BF16)] * 2
        + [jax.ShapeDtypeStruct((num_loc, width, model), BF16)],
        compiler_params=pltpu.CompilerParams(dimension_semantics=('arbitrary',)),
        cost_estimate=pl.CostEstimate(flops=6 * num_loc * slots * model * width,
                                      bytes_accessed=50 * 2 ** 20, transcendentals=0),
        name='weight_grads',
    )(tall, wide)


def solution(mesh):
    group = mesh.shape['expert']
    stages = mesh.shape['stage']

    def device_fn(x_acts, expert_ids, gate_wts, w_in, w_up, w_out, d_out):
        num_loc = w_in.shape[1]
        tokens = x_acts.shape[2]
        top_k = expert_ids.shape[3]
        cap = 3 * top_k * tokens // (2 * num_loc * group)
        ids = jnp.swapaxes(expert_ids[:, 0], 1, 2)
        gates = jnp.swapaxes(gate_wts[:, 0], 1, 2)
        dx_home, y_loc, y_x, wide, tall = stage_call(
            stages, cap, ids, gates, x_acts, d_out, w_in, w_up, w_out)
        d_x = lax.ppermute(dx_home, 'stage', [((s + 1) % stages, s) for s in range(stages)])
        y_in = lax.ppermute(y_x, 'expert', [(i, i ^ 2) for i in range(group)])
        d_in, d_up, d_wout = weight_call(wide, tall)
        y = (y_loc.astype(F32) + y_in.astype(F32)).astype(BF16)
        return y[None], d_x[None], d_in[None], d_up[None], d_wout[None]

    tok_spec = P(None, 'stage', 'expert', None)
    w_spec = P('stage', 'expert', None, None)
    row_spec = P('stage', 'expert', None)
    return jax.shard_map(device_fn, mesh=mesh,
                         in_specs=(tok_spec, tok_spec, tok_spec, w_spec, w_spec, w_spec, row_spec),
                         out_specs=(row_spec, row_spec, w_spec, w_spec, w_spec), check_vma=False)
```

```python
import functools

import jax
import jax.numpy as jnp
from jax import lax
from jax.experimental import pallas as pl
from jax.experimental.pallas import tpu as pltpu
from jax.sharding import PartitionSpec as P

BF16 = jnp.bfloat16
F32 = jnp.float32
MESH = pl.DeviceIdType.MESH
TILE = 256
PARTS = 4
EARLY = 2
A, B, A_FAR, B_FAR = range(4)


def dot(lhs, rhs, lc=1, rc=0):
    return lax.dot_general(lhs, rhs, (((lc,), (rc,)), ((), ())), preferred_element_type=F32)


def routing(mb, num_loc, ids, gates, pos, gate_rows, pos_cols):
    first = lax.axis_index('expert') * num_loc
    tokens = ids.shape[-1]
    rows = 4 * num_loc
    lane = lax.broadcasted_iota(jnp.int32, (rows, tokens), 1)
    sub = lax.broadcasted_iota(jnp.int32, (rows, tokens), 0)
    expert = first + sub % num_loc

    def field(ref, k):
        return jnp.concatenate([ref[s, mb, k:k + 1, :] for s in range(4) for _ in range(num_loc)], axis=0)

    hit0, hit1 = field(ids, 0) == expert, field(ids, 1) == expert
    gate_rows[mb] = jnp.where(hit0, field(gates, 0), 0.0) + jnp.where(hit1, field(gates, 1), 0.0)
    taken = jnp.where(hit0 | hit1, 1, 0)
    run = taken
    step = 1
    while step < tokens:
        run = run + jnp.where(lane >= step, pltpu.roll(run, step, 1), 0)
        step *= 2
    slot = jnp.where(taken == 1, run - 1, -1)
    pos[mb] = slot
    pos_cols[mb, :, 0:rows] = slot.T


def pick(pos, gate_rows, mb, row, cap):
    tokens = pos.shape[-1]
    hit = pos[mb, pl.ds(row, 1), :] == lax.broadcasted_iota(jnp.int32, (cap, tokens), 0)
    gate = jnp.sum(jnp.where(hit, gate_rows[mb, pl.ds(row, 1), :], 0.0), axis=1, keepdims=True)
    return jnp.where(hit, 1.0, 0.0).astype(BF16), gate


def to_tokens(pos_cols, mb, block, rows, out):
    num_loc, cap, _ = rows.shape
    part = out.shape[2] // PARTS
    for m in range(PARTS):
        span = slice(m * part, (m + 1) * part)
        cols = pltpu.roll(pos_cols[mb, span, :], lax.rem(128 - num_loc * block, 128), 1)
        slot = lax.broadcasted_iota(jnp.int32, (part, cap), 1)
        sel = [jnp.where(cols[:, e:e + 1] == slot, 1.0, 0.0).astype(BF16) for e in range(num_loc)]
        total = dot(jnp.concatenate(sel, axis=1), rows[...].reshape(num_loc * cap, rows.shape[2]))
        out[mb, block, span, :] = total.astype(BF16)


def add_bf16(*refs):
    total = refs[0][...].astype(F32)
    for ref in refs[1:]:
        total += ref[...].astype(F32)
    return total.astype(BF16)


def stage_kernel(num_stages, cap, ids_in, gates_in, x_hbm, dy_hbm, win_hbm, wup_hbm, wout_hbm,
                 dx_hbm, y_hbm, yx_hbm, wide_hbm, tall_hbm,
                 ids, gates, xs, dys, win, wup, wout, pos, gate_rows, pos_cols, rows, ret, rin, cin,
                 wide_buf, tall_buf, q_early, u_early,
                 meta_send, meta_recv, hop_send, hop_recv, fwd_send, fwd_recv, dy_sem, dy_send, dy_recv,
                 ret_send, ret_recv, crs_send, crs_recv, w_sem, out_sem, res_sem, pace):
    stage, me = lax.axis_index('stage'), lax.axis_index('expert')
    nxt, prv = lax.rem(stage + 1, num_stages), lax.rem(stage + num_stages - 1, num_stages)
    core, chip = lax.rem(me, 2), me // 2
    other = 1 - core

    def peer(flip):
        new_core = other if flip % 2 else core
        new_chip = 1 - chip if flip // 2 else chip
        return 2 * new_chip + new_core

    partner, across = (stage, peer(1)), (stage, peer(2))
    num_loc, model, width = win.shape
    tokens = xs.shape[2]
    part = tokens // PARTS
    tiles = width // TILE

    def remote(src, dst, send, recv, device):
        return pltpu.make_async_remote_copy(src_ref=src, dst_ref=dst, send_sem=send, recv_sem=recv,
                                            device_id=device, device_id_type=MESH)

    def meta(flip, k, block=None):
        src, dst = ((ids_in, ids), (gates_in, gates))[k]
        block = 2 * (flip // 2) + core if block is None else block
        return remote(src, dst.at[block], meta_send.at[k, flip], meta_recv.at[k, block], (nxt, peer(flip)))

    def piece(mb, block, k):
        return xs.at[mb, block, pl.ds(k * part, part)]

    def hop(mb, k):
        src = x_hbm.at[mb, 0, pl.ds(k * part, part)]
        return remote(src, piece(mb, core, k), hop_send.at[mb, k], hop_recv.at[mb, k], (nxt, me))

    def near(mb, k, block=None):
        ref = piece(mb, core if block is None else block, k)
        return remote(ref, ref, fwd_send.at[mb, 0, k], fwd_recv.at[mb, 0, k], partner)

    def cross(mb, k):
        return remote(piece(mb, core, k), piece(mb, 2 + core, k), fwd_send.at[mb, 1, k], fwd_recv.at[mb, 1, k],
                      across)

    def far(mb, k, block=None):
        ref = piece(mb, 2 + core if block is None else block, k)
        return remote(ref, ref, fwd_send.at[mb, 2, k], fwd_recv.at[mb, 2, k], partner)

    def near_arrived(mb):
        for k in range(PARTS):
            near(mb, k, other).wait_recv()

    def far_arrived(mb):
        for k in range(PARTS):
            far(mb, k, 2 + other).wait_recv()

    dy_own = pltpu.make_async_copy(dy_hbm.at[0], dys.at[core], dy_sem)
    dy_near = remote(dy_hbm.at[0], dys.at[core], dy_send.at[0], dy_recv.at[0], partner)
    dy_near_in = remote(dy_hbm.at[0], dys.at[other], dy_send.at[0], dy_recv.at[0], partner)
    dy_cross = remote(dy_hbm.at[0], dys.at[2 + core], dy_send.at[1], dy_recv.at[1], across)
    dy_far = remote(dys.at[2 + core], dys.at[2 + core], dy_send.at[2], dy_recv.at[2], partner)
    dy_far_in = remote(dys.at[2 + other], dys.at[2 + other], dy_send.at[2], dy_recv.at[2], partner)

    def back(mb, k, block=None):
        src = ret.at[mb, 2 * k + other if block is None else block]
        return remote(src, rin.at[mb, k], ret_send.at[mb, k], ret_recv.at[mb, k], partner)

    def send_back(mb, block):
        @pl.when(lax.rem(block, 2) != core)
        def _():
            back(mb, block // 2, block).start()

    dx_cross = remote(ret.at[0, 2 + core], cin, crs_send, crs_recv, across)

    def dx_across():
        back(0, 1).wait_recv()
        ret[0, 2 + core] = add_bf16(ret.at[0, 2 + core], rin.at[0, 1])
        dx_cross.start()

    dx_save = pltpu.make_async_copy(ret.at[0, core], dx_hbm, res_sem.at[0])
    y_save = pltpu.make_async_copy(ret.at[1, core], y_hbm, res_sem.at[1])
    yx_save = pltpu.make_async_copy(ret.at[1, 2 + core], yx_hbm, res_sem.at[2])

    weights = [pltpu.make_async_copy(src.at[0], dst, w_sem.at[k])
               for k, (src, dst) in enumerate(((win_hbm, win), (wup_hbm, wup), (wout_hbm, wout)))]

    def outs(st):
        slot = lax.rem(st, 2)
        block, e = st // num_loc, lax.rem(st, num_loc)
        span = pl.ds(pl.multiple_of(block * cap, cap), cap)
        return (pltpu.make_async_copy(wide_buf.at[slot], wide_hbm.at[e, :, :, span], out_sem.at[slot, 0]),
                pltpu.make_async_copy(tall_buf.at[slot], tall_hbm.at[e, :, :, span], out_sem.at[slot, 1]))

    def at(now, when, on_core=None):
        cond = now == when if on_core is None else (now == when) & (core == on_core)
        return pl.when(cond)

    barrier = pltpu.get_barrier_semaphore()
    for device in [(prv, peer(flip)) for flip in range(4)] + [partner, across]:
        pl.semaphore_signal(barrier, inc=1, device_id=device, device_id_type=MESH)
    pl.semaphore_wait(barrier, 6)

    for flip in range(4):
        for k in range(2):
            meta(flip, k).start()

    @pl.when(core == 0)
    def _():
        for k in range(PARTS):
            hop(0, k).start()
        dy_cross.start()

    dy_near.start()
    dy_own.start()
    for copy in weights:
        copy.start()

    for block in range(4):
        for k in range(2):
            meta(0, k, block).wait_recv()
    for mb in range(2):
        routing(mb, num_loc, ids, gates, pos, gate_rows, pos_cols)
    dy_own.wait()
    dy_near_in.wait_recv()
    for copy in weights:
        copy.wait()

    def cotangent(st):
        sel, gate = pick(pos, gate_rows, 0, st, cap)
        return sel, gate * dot(sel, dys[st // num_loc])

    def early_step(st, carry):
        q = cotangent(st)[1].astype(BF16)
        q_early[st] = q
        for t in range(tiles):
            cols = slice(t * TILE, (t + 1) * TILE)
            u_early[st, :, cols] = dot(q, wout[lax.rem(st, num_loc), cols, :], 1, 1)
        return carry

    lax.fori_loop(0, EARLY, early_step, 0)

    @pl.when(core == 0)
    def _():
        for k in range(PARTS):
            hop(0, k).wait_recv()
            near(0, k).start()
            cross(0, k).start()
            if k == PARTS - 2:
                pl.semaphore_signal(pace, inc=1, device_id=partner, device_id_type=MESH)

    @pl.when(core == 1)
    def _():
        pl.semaphore_wait(pace, 1)
        for k in range(PARTS):
            hop(0, k).start()
        dy_cross.start()
        near_arrived(0)

    steps = 4 * num_loc
    half, most = PARTS // 2, PARTS - 1

    def pass_on(mb, lo, hi):
        for k in range(lo, hi):
            hop(mb, k).wait_recv()
            near(mb, k).start()
            cross(mb, k).start()

    def pass_far(mb, lo, hi):
        for k in range(lo, hi):
            cross(mb, k).wait_recv()
            far(mb, k).start()

    def backward_step(early, st, carry):
        block, e = st // num_loc, lax.rem(st, num_loc)
        slot = lax.rem(st, 2)

        @at(st, 1, on_core=1)
        def _():
            pass_on(0, 0, most)

        @at(st, num_loc, on_core=1)
        def _():
            pass_on(0, most, PARTS)

        @at(st, num_loc, on_core=0)
        def _():
            for k in range(PARTS):
                hop(1, k).start()
            near_arrived(0)

        @at(st, num_loc + 1, on_core=0)
        def _():
            dy_cross.wait_recv()
            dy_far.start()
            pass_far(0, 0, PARTS)

        @at(st, 2 * num_loc, on_core=0)
        def _():
            pass_on(1, 0, half)

        @at(st, 2 * num_loc, on_core=1)
        def _():
            for k in range(PARTS):
                hop(1, k).start()
            far_arrived(0)
            dy_far_in.wait_recv()

        @at(st, 2 * num_loc + 1, on_core=0)
        def _():
            pass_on(1, half, PARTS)

        @at(st, 2 * num_loc + 1, on_core=1)
        def _():
            dy_cross.wait_recv()
            dy_far.start()
            pass_far(0, 0, most)

        @at(st, 3 * num_loc, on_core=1)
        def _():
            pass_far(0, most, PARTS)
            pass_on(1, 0, half)

        @at(st, 3 * num_loc, on_core=0)
        def _():
            far_arrived(0)
            dy_far_in.wait_recv()

        @at(st, 3 * num_loc + 1, on_core=1)
        def _():
            pass_on(1, half, PARTS)

        @at(st, 3 * num_loc + 1, on_core=0)
        def _():
            dx_across()

        @pl.when(st >= 2)
        def _():
            for copy in outs(st - 2):
                copy.wait()

        if early:
            sel = pick(pos, gate_rows, 0, st, cap)[0]
            gdy = q_early[st].astype(F32)
        else:
            sel, gdy = cotangent(st)
        x = dot(sel, xs[0, block])
        tall_buf[slot, 0] = x.T.astype(BF16)
        tall_buf[slot, 1] = gdy.T.astype(BF16)
        x, q = x.astype(BF16), gdy.astype(BF16)
        for t in range(tiles):
            cols = slice(t * TILE, (t + 1) * TILE)
            a = dot(x, win[e, :, cols])
            b = dot(x, wup[e, :, cols])
            u = u_early[st, :, cols] if early else dot(q, wout[e, cols, :], 1, 1)
            sig = jax.nn.sigmoid(a)
            act = a * sig
            wide_buf[slot, t, 0] = (u * b * sig * (1.0 + a * (1.0 - sig))).astype(BF16)
            wide_buf[slot, t, 1] = (u * act).astype(BF16)
            wide_buf[slot, t, 2] = (act * b).astype(BF16)
        g_in = jnp.concatenate([wide_buf[slot, t, 0] for t in range(tiles)], axis=1)
        g_up = jnp.concatenate([wide_buf[slot, t, 1] for t in range(tiles)], axis=1)
        rows[e] = (dot(g_in, win[e], 1, 1) + dot(g_up, wup[e], 1, 1)).astype(BF16)
        for copy in outs(st):
            copy.start()

        @pl.when(e == num_loc - 1)
        def _():
            to_tokens(pos_cols, 0, block, rows, ret)
            send_back(0, block)

        return carry

    lax.fori_loop(0, EARLY, functools.partial(backward_step, True), 0)
    lax.fori_loop(EARLY, steps, functools.partial(backward_step, False), 0)
    for copy in outs(steps - 2):
        copy.wait()

    def forward_step(st, carry):
        block, e = st // num_loc, lax.rem(st, num_loc)

        @at(st, 0, on_core=1)
        def _():
            near_arrived(1)

        @at(st, 1, on_core=1)
        def _():
            dx_across()

        @at(st, num_loc, on_core=0)
        def _():
            near_arrived(1)

        @at(st, num_loc + 1, on_core=0)
        def _():
            pass_far(1, 0, PARTS)

        @at(st, 2 * num_loc, on_core=1)
        def _():
            far_arrived(1)

        @at(st, 2 * num_loc + 1, on_core=1)
        def _():
            pass_far(1, 0, most)

        @at(st, 3 * num_loc, on_core=1)
        def _():
            pass_far(1, most, PARTS)

        @at(st, 3 * num_loc)
        def _():
            back(1, 0).wait_recv()
            ret[1, core] = add_bf16(ret.at[1, core], rin.at[1, 0])
            y_save.start()

        @at(st, 3 * num_loc, on_core=0)
        def _():
            far_arrived(1)

        sel, gate = pick(pos, gate_rows, 1, st, cap)
        x = dot(sel, xs[1, block]).astype(BF16)
        for t in range(tiles):
            cols = slice(t * TILE, (t + 1) * TILE)
            a = dot(x, win[e, :, cols])
            b = dot(x, wup[e, :, cols])
            wide_buf[0, t, 0] = (a * jax.nn.sigmoid(a) * b).astype(BF16)
        hid = jnp.concatenate([wide_buf[0, t, 0] for t in range(tiles)], axis=1)
        rows[e] = (gate * dot(hid, wout[e])).astype(BF16)

        @pl.when(e == num_loc - 1)
        def _():
            to_tokens(pos_cols, 1, block, rows, ret)
            send_back(1, block)

        return carry

    lax.fori_loop(0, steps, forward_step, 0)
    back(1, 1).wait_recv()
    ret[1, 2 + core] = add_bf16(ret.at[1, 2 + core], rin.at[1, 1])
    yx_save.start()
    back(0, 0).wait_recv()
    dx_cross.wait_recv()
    ret[0, core] = add_bf16(ret.at[0, core], rin.at[0, 0], cin)
    dx_save.start()

    for copy in outs(steps - 1):
        copy.wait()
    for flip in range(4):
        for k in range(2):
            meta(flip, k).wait_send()
    for mb in range(2):
        for k in range(PARTS):
            hop(mb, k).wait_send()
            near(mb, k).wait_send()
            cross(mb, k).wait_send()
            far(mb, k).wait_send()
        for k in range(2):
            back(mb, k).wait_send()
    for copy in (dy_near, dy_cross, dy_far, dx_cross):
        copy.wait_send()
    for copy in (y_save, yx_save, dx_save):
        copy.wait()


def stage_call(num_stages, cap, ids, gates, x_acts, d_out, w_in, w_up, w_out):
    _, num_loc, model, width = w_in.shape
    tokens = x_acts.shape[2]
    slots = 4 * cap
    whole = pl.BlockSpec(memory_space=pltpu.VMEM)
    anyspace = pl.BlockSpec(memory_space=pl.ANY)
    block = jax.ShapeDtypeStruct((tokens, model), BF16)
    wide = jax.ShapeDtypeStruct((num_loc, width // TILE, 3, slots, TILE), BF16)
    tall = jax.ShapeDtypeStruct((num_loc, 2, model, slots), BF16)
    vmem = pltpu.VMEM
    dma = pltpu.SemaphoreType.DMA
    return pl.pallas_call(
        functools.partial(stage_kernel, num_stages, cap),
        out_shape=[block] * 3 + [wide, tall],
        in_specs=[whole] * 2 + [anyspace] * 5,
        out_specs=[anyspace] * 5,
        scratch_shapes=[
            vmem((4,) + ids.shape, jnp.int32), vmem((4,) + gates.shape, F32),
            vmem((2, 4, tokens, model), BF16), vmem((4, tokens, model), BF16),
            vmem((num_loc, model, width), BF16), vmem((num_loc, model, width), BF16),
            vmem((num_loc, width, model), BF16),
            vmem((2, 4 * num_loc, tokens), jnp.int32), vmem((2, 4 * num_loc, tokens), F32),
            vmem((2, tokens, 128), jnp.int32),
            vmem((num_loc, cap, model), BF16), vmem((2, 4, tokens, model), BF16),
            vmem((2, 2, tokens, model), BF16), vmem((tokens, model), BF16),
            vmem((2, width // TILE, 3, cap, TILE), BF16), vmem((2, 2, model, cap), BF16),
            vmem((EARLY, cap, model), BF16), vmem((EARLY, cap, width), F32),
            dma((2, 4)), dma((2, 4)), dma((2, PARTS)), dma((2, PARTS)), dma((2, 3, PARTS)), dma((2, 3, PARTS)),
            dma, dma((3,)), dma((3,)), dma((2, 2)), dma((2, 2)), dma, dma, dma((3,)), dma((2, 2)), dma((3,)),
            pltpu.SemaphoreType.REGULAR,
        ],
        compiler_params=pltpu.CompilerParams(collective_id=0, has_side_effects=True, vmem_limit_bytes=66_500_000),
        cost_estimate=pl.CostEstimate(flops=16 * num_loc * slots * model * width,
                                      bytes_accessed=70 * 2 ** 20, transcendentals=0),
        name='stage_layer',
    )(ids, gates, x_acts, d_out, w_in, w_up, w_out)


def weight_kernel(tall, wide, din_ref, dup_ref, dout_ref):
    for e in range(tall.shape[0]):
        din_ref[e] = dot(tall[e, 0], wide[e, 0, 0]).astype(BF16)
        dup_ref[e] = dot(tall[e, 0], wide[e, 0, 1]).astype(BF16)
        dout_ref[e] = dot(tall[e, 1], wide[e, 0, 2]).T.astype(BF16)


def weight_call(wide, tall):
    num_loc, tiles, _, slots, _ = wide.shape
    model, width = tall.shape[2], tiles * TILE
    return pl.pallas_call(
        weight_kernel,
        grid=(tiles,),
        in_specs=[pl.BlockSpec(tall.shape, lambda t: (0, 0, 0, 0)),
                  pl.BlockSpec((num_loc, 1, 3, slots, TILE), lambda t: (0, t, 0, 0, 0))],
        out_specs=[pl.BlockSpec((num_loc, model, TILE), lambda t: (0, 0, t))] * 2
        + [pl.BlockSpec((num_loc, TILE, model), lambda t: (0, t, 0))],
        out_shape=[jax.ShapeDtypeStruct((num_loc, model, width), BF16)] * 2
        + [jax.ShapeDtypeStruct((num_loc, width, model), BF16)],
        compiler_params=pltpu.CompilerParams(dimension_semantics=('arbitrary',)),
        cost_estimate=pl.CostEstimate(flops=6 * num_loc * slots * model * width,
                                      bytes_accessed=50 * 2 ** 20, transcendentals=0),
        name='weight_grads',
    )(tall, wide)


def solution(mesh):
    group = mesh.shape['expert']
    stages = mesh.shape['stage']

    def device_fn(x_acts, expert_ids, gate_wts, w_in, w_up, w_out, d_out):
        num_loc = w_in.shape[1]
        tokens = x_acts.shape[2]
        top_k = expert_ids.shape[3]
        cap = 3 * top_k * tokens // (2 * num_loc * group)
        ids = jnp.swapaxes(expert_ids[:, 0], 1, 2)
        gates = jnp.swapaxes(gate_wts[:, 0], 1, 2)
        dx_home, y_loc, y_x, wide, tall = stage_call(
            stages, cap, ids, gates, x_acts, d_out, w_in, w_up, w_out)
        d_x = lax.ppermute(dx_home, 'stage', [((s + 1) % stages, s) for s in range(stages)])
        y_in = lax.ppermute(y_x, 'expert', [(i, i ^ 2) for i in range(group)])
        d_in, d_up, d_wout = weight_call(wide, tall)
        y = (y_loc.astype(F32) + y_in.astype(F32)).astype(BF16)
        return y[None], d_x[None], d_in[None], d_up[None], d_wout[None]

    tok_spec = P(None, 'stage', 'expert', None)
    w_spec = P('stage', 'expert', None, None)
    row_spec = P('stage', 'expert', None)
    return jax.shard_map(device_fn, mesh=mesh,
                         in_specs=(tok_spec, tok_spec, tok_spec, w_spec, w_spec, w_spec, row_spec),
                         out_specs=(row_spec, row_spec, w_spec, w_spec, w_spec), check_vma=False)
```

```python
import functools

import jax
import jax.numpy as jnp
from jax import lax
from jax.experimental import pallas as pl
from jax.experimental.pallas import tpu as pltpu
from jax.sharding import PartitionSpec as P

BF16 = jnp.bfloat16
F32 = jnp.float32
MESH = pl.DeviceIdType.MESH
TILE = 256
PARTS = 4
EARLY = 2
A, B, A_FAR, B_FAR = range(4)


def dot(lhs, rhs, lc=1, rc=0):
    return lax.dot_general(lhs, rhs, (((lc,), (rc,)), ((), ())), preferred_element_type=F32)


def routing(mb, num_loc, ids, gates, pos, gate_rows, pos_cols):
    first = lax.axis_index('expert') * num_loc
    tokens = ids.shape[-1]
    rows = 4 * num_loc
    lane = lax.broadcasted_iota(jnp.int32, (rows, tokens), 1)
    sub = lax.broadcasted_iota(jnp.int32, (rows, tokens), 0)
    expert = first + sub % num_loc

    def field(ref, k):
        return jnp.concatenate([ref[s, mb, k:k + 1, :] for s in range(4) for _ in range(num_loc)], axis=0)

    hit0, hit1 = field(ids, 0) == expert, field(ids, 1) == expert
    gate_rows[mb] = jnp.where(hit0, field(gates, 0), 0.0) + jnp.where(hit1, field(gates, 1), 0.0)
    taken = jnp.where(hit0 | hit1, 1, 0)
    run = taken
    step = 1
    while step < tokens:
        run = run + jnp.where(lane >= step, pltpu.roll(run, step, 1), 0)
        step *= 2
    slot = jnp.where(taken == 1, run - 1, -1)
    pos[mb] = slot
    pos_cols[mb, :, 0:rows] = slot.T


def pick(pos, gate_rows, mb, row, cap):
    tokens = pos.shape[-1]
    hit = pos[mb, pl.ds(row, 1), :] == lax.broadcasted_iota(jnp.int32, (cap, tokens), 0)
    gate = jnp.sum(jnp.where(hit, gate_rows[mb, pl.ds(row, 1), :], 0.0), axis=1, keepdims=True)
    return jnp.where(hit, 1.0, 0.0).astype(BF16), gate


def to_tokens(pos_cols, mb, block, rows, out):
    num_loc, cap, _ = rows.shape
    part = out.shape[2] // PARTS
    for m in range(PARTS):
        span = slice(m * part, (m + 1) * part)
        slot = lax.broadcasted_iota(jnp.int32, (part, cap), 1)
        cols = [pos_cols[mb, span, num_loc * block + e:num_loc * block + e + 1] for e in range(num_loc)]
        sel = [jnp.where(col == slot, 1.0, 0.0).astype(BF16) for col in cols]
        total = dot(jnp.concatenate(sel, axis=1), rows[...].reshape(num_loc * cap, rows.shape[2]))
        out[mb, block, span, :] = total.astype(BF16)


def add_bf16(*refs):
    total = refs[0][...].astype(F32)
    for ref in refs[1:]:
        total += ref[...].astype(F32)
    return total.astype(BF16)


def stage_kernel(num_stages, cap, ids_in, gates_in, x_hbm, dy_hbm, win_hbm, wup_hbm, wout_hbm,
                 dx_hbm, y_hbm, yx_hbm, wide_hbm, tall_hbm,
                 ids, gates, xs, dys, win, wup, wout, pos, gate_rows, pos_cols, rows, ret, rin, cin,
                 wide_buf, tall_buf, q_early, u_early,
                 meta_send, meta_recv, hop_send, hop_recv, fwd_send, fwd_recv, dy_sem, dy_send, dy_recv,
                 ret_send, ret_recv, crs_send, crs_recv, w_sem, out_sem, res_sem, pace):
    stage, me = lax.axis_index('stage'), lax.axis_index('expert')
    nxt, prv = lax.rem(stage + 1, num_stages), lax.rem(stage + num_stages - 1, num_stages)
    core, chip = lax.rem(me, 2), me // 2
    other = 1 - core

    def peer(flip):
        new_core = other if flip % 2 else core
        new_chip = 1 - chip if flip // 2 else chip
        return 2 * new_chip + new_core

    partner, across = (stage, peer(1)), (stage, peer(2))
    num_loc, model, width = win.shape
    tokens = xs.shape[2]
    part = tokens // PARTS
    tiles = width // TILE

    def remote(src, dst, send, recv, device):
        return pltpu.make_async_remote_copy(src_ref=src, dst_ref=dst, send_sem=send, recv_sem=recv,
                                            device_id=device, device_id_type=MESH)

    def meta(flip, k, block=None):
        src, dst = ((ids_in, ids), (gates_in, gates))[k]
        block = 2 * (flip // 2) + core if block is None else block
        return remote(src, dst.at[block], meta_send.at[k, flip], meta_recv.at[k, block], (nxt, peer(flip)))

    def piece(mb, block, k):
        return xs.at[mb, block, pl.ds(k * part, part)]

    def hop(mb, k):
        src = x_hbm.at[mb, 0, pl.ds(k * part, part)]
        return remote(src, piece(mb, core, k), hop_send.at[mb, k], hop_recv.at[mb, k], (nxt, me))

    def near(mb, k, block=None):
        ref = piece(mb, core if block is None else block, k)
        return remote(ref, ref, fwd_send.at[mb, 0, k], fwd_recv.at[mb, 0, k], partner)

    def cross(mb, k):
        return remote(piece(mb, core, k), piece(mb, 2 + core, k), fwd_send.at[mb, 1, k], fwd_recv.at[mb, 1, k],
                      across)

    def far(mb, k, block=None):
        ref = piece(mb, 2 + core if block is None else block, k)
        return remote(ref, ref, fwd_send.at[mb, 2, k], fwd_recv.at[mb, 2, k], partner)

    def near_arrived(mb):
        for k in range(PARTS):
            near(mb, k, other).wait_recv()

    def far_arrived(mb):
        for k in range(PARTS):
            far(mb, k, 2 + other).wait_recv()

    dy_own = pltpu.make_async_copy(dy_hbm.at[0], dys.at[core], dy_sem)
    dy_near = remote(dy_hbm.at[0], dys.at[core], dy_send.at[0], dy_recv.at[0], partner)
    dy_near_in = remote(dy_hbm.at[0], dys.at[other], dy_send.at[0], dy_recv.at[0], partner)
    dy_cross = remote(dy_hbm.at[0], dys.at[2 + core], dy_send.at[1], dy_recv.at[1], across)
    dy_far = remote(dys.at[2 + core], dys.at[2 + core], dy_send.at[2], dy_recv.at[2], partner)
    dy_far_in = remote(dys.at[2 + other], dys.at[2 + other], dy_send.at[2], dy_recv.at[2], partner)

    def back(mb, k, block=None):
        src = ret.at[mb, 2 * k + other if block is None else block]
        return remote(src, rin.at[mb, k], ret_send.at[mb, k], ret_recv.at[mb, k], partner)

    def finish_block(mb, st, blocks):
        for block in blocks:
            @pl.when(st == (block + 1) * num_loc - 1)
            def _(block=block):
                to_tokens(pos_cols, mb, block, rows, ret)

                @pl.when(core != block % 2)
                def _():
                    back(mb, block // 2, block).start()

    dx_cross = remote(ret.at[0, 2 + core], cin, crs_send, crs_recv, across)

    def dx_across():
        back(0, 1).wait_recv()
        ret[0, 2 + core] = add_bf16(ret.at[0, 2 + core], rin.at[0, 1])
        dx_cross.start()

    dx_save = pltpu.make_async_copy(ret.at[0, core], dx_hbm, res_sem.at[0])
    y_save = pltpu.make_async_copy(ret.at[1, core], y_hbm, res_sem.at[1])
    yx_save = pltpu.make_async_copy(ret.at[1, 2 + core], yx_hbm, res_sem.at[2])

    weights = [pltpu.make_async_copy(src.at[0], dst, w_sem.at[k])
               for k, (src, dst) in enumerate(((win_hbm, win), (wup_hbm, wup), (wout_hbm, wout)))]

    def outs(st):
        slot = lax.rem(st, 2)
        block, e = st // num_loc, lax.rem(st, num_loc)
        span = pl.ds(pl.multiple_of(block * cap, cap), cap)
        return (pltpu.make_async_copy(wide_buf.at[slot], wide_hbm.at[e, :, :, span], out_sem.at[slot, 0]),
                pltpu.make_async_copy(tall_buf.at[slot], tall_hbm.at[e, :, :, span], out_sem.at[slot, 1]))

    def at(now, when, on_core=None):
        cond = now == when if on_core is None else (now == when) & (core == on_core)
        return pl.when(cond)

    barrier = pltpu.get_barrier_semaphore()
    for device in [(prv, peer(flip)) for flip in range(4)] + [partner, across]:
        pl.semaphore_signal(barrier, inc=1, device_id=device, device_id_type=MESH)
    pl.semaphore_wait(barrier, 6)

    for flip in range(4):
        for k in range(2):
            meta(flip, k).start()

    @pl.when(core == 0)
    def _():
        for k in range(PARTS):
            hop(0, k).start()
        dy_cross.start()

    dy_near.start()
    dy_own.start()
    for copy in weights:
        copy.start()

    for block in range(4):
        for k in range(2):
            meta(0, k, block).wait_recv()
    for mb in range(2):
        routing(mb, num_loc, ids, gates, pos, gate_rows, pos_cols)
    dy_own.wait()
    dy_near_in.wait_recv()
    for copy in weights:
        copy.wait()

    def cotangent(st):
        sel, gate = pick(pos, gate_rows, 0, st, cap)
        return sel, gate * dot(sel, dys[st // num_loc])

    def early_step(st, carry):
        q = cotangent(st)[1].astype(BF16)
        q_early[st] = q
        for t in range(tiles):
            cols = slice(t * TILE, (t + 1) * TILE)
            u_early[st, :, cols] = dot(q, wout[lax.rem(st, num_loc), cols, :], 1, 1)
        return carry

    lax.fori_loop(0, EARLY, early_step, 0)

    @pl.when(core == 0)
    def _():
        for k in range(PARTS):
            hop(0, k).wait_recv()
            near(0, k).start()
            cross(0, k).start()
            if k == PARTS - 2:
                pl.semaphore_signal(pace, inc=1, device_id=partner, device_id_type=MESH)

    @pl.when(core == 1)
    def _():
        pl.semaphore_wait(pace, 1)
        for k in range(PARTS):
            hop(0, k).start()
        dy_cross.start()
        near_arrived(0)

    steps = 4 * num_loc
    half, most = PARTS // 2, PARTS - 1

    def pass_on(mb, lo, hi):
        for k in range(lo, hi):
            hop(mb, k).wait_recv()
            near(mb, k).start()
            cross(mb, k).start()

    def pass_far(mb, lo, hi):
        for k in range(lo, hi):
            cross(mb, k).wait_recv()
            far(mb, k).start()

    def backward_step(early, st, carry):
        block, e = st // num_loc, lax.rem(st, num_loc)
        slot = lax.rem(st, 2)

        @at(st, 1, on_core=1)
        def _():
            pass_on(0, 0, most)

        @at(st, num_loc, on_core=1)
        def _():
            pass_on(0, most, PARTS)

        @at(st, num_loc, on_core=0)
        def _():
            for k in range(PARTS):
                hop(1, k).start()
            near_arrived(0)

        @at(st, num_loc + 1, on_core=0)
        def _():
            dy_cross.wait_recv()
            dy_far.start()
            pass_far(0, 0, PARTS)

        @at(st, 2 * num_loc, on_core=0)
        def _():
            pass_on(1, 0, half)

        @at(st, 2 * num_loc, on_core=1)
        def _():
            for k in range(PARTS):
                hop(1, k).start()
            far_arrived(0)
            dy_far_in.wait_recv()

        @at(st, 2 * num_loc + 1, on_core=0)
        def _():
            pass_on(1, half, PARTS)

        @at(st, 2 * num_loc + 1, on_core=1)
        def _():
            dy_cross.wait_recv()
            dy_far.start()
            pass_far(0, 0, most)

        @at(st, 3 * num_loc, on_core=1)
        def _():
            pass_far(0, most, PARTS)
            pass_on(1, 0, half)

        @at(st, 3 * num_loc, on_core=0)
        def _():
            far_arrived(0)
            dy_far_in.wait_recv()

        @at(st, 3 * num_loc + 1, on_core=1)
        def _():
            pass_on(1, half, PARTS)

        @at(st, 3 * num_loc + 1, on_core=0)
        def _():
            dx_across()

        @pl.when(st >= 2)
        def _():
            for copy in outs(st - 2):
                copy.wait()

        if early:
            sel = pick(pos, gate_rows, 0, st, cap)[0]
            gdy = q_early[st].astype(F32)
        else:
            sel, gdy = cotangent(st)
        x = dot(sel, xs[0, block])
        tall_buf[slot, 0] = x.T.astype(BF16)
        tall_buf[slot, 1] = gdy.T.astype(BF16)
        x, q = x.astype(BF16), gdy.astype(BF16)
        for t in range(tiles):
            cols = slice(t * TILE, (t + 1) * TILE)
            a = dot(x, win[e, :, cols])
            b = dot(x, wup[e, :, cols])
            u = u_early[st, :, cols] if early else dot(q, wout[e, cols, :], 1, 1)
            sig = jax.nn.sigmoid(a)
            act = a * sig
            wide_buf[slot, t, 0] = (u * b * sig * (1.0 + a * (1.0 - sig))).astype(BF16)
            wide_buf[slot, t, 1] = (u * act).astype(BF16)
            wide_buf[slot, t, 2] = (act * b).astype(BF16)
        g_in = jnp.concatenate([wide_buf[slot, t, 0] for t in range(tiles)], axis=1)
        g_up = jnp.concatenate([wide_buf[slot, t, 1] for t in range(tiles)], axis=1)
        rows[e] = (dot(g_in, win[e], 1, 1) + dot(g_up, wup[e], 1, 1)).astype(BF16)
        for copy in outs(st):
            copy.start()

        finish_block(0, st, range(EARLY // num_loc) if early else range(EARLY // num_loc, 4))

        return carry

    lax.fori_loop(0, EARLY, functools.partial(backward_step, True), 0)
    lax.fori_loop(EARLY, steps, functools.partial(backward_step, False), 0)
    for copy in outs(steps - 2):
        copy.wait()

    def forward_step(st, carry):
        block, e = st // num_loc, lax.rem(st, num_loc)

        @at(st, 0, on_core=1)
        def _():
            near_arrived(1)

        @at(st, 1, on_core=1)
        def _():
            dx_across()

        @at(st, num_loc, on_core=0)
        def _():
            near_arrived(1)

        @at(st, num_loc + 1, on_core=0)
        def _():
            pass_far(1, 0, PARTS)

        @at(st, 2 * num_loc, on_core=1)
        def _():
            far_arrived(1)

        @at(st, 2 * num_loc + 1, on_core=1)
        def _():
            pass_far(1, 0, most)

        @at(st, 3 * num_loc, on_core=1)
        def _():
            pass_far(1, most, PARTS)

        @at(st, 3 * num_loc)
        def _():
            back(1, 0).wait_recv()
            ret[1, core] = add_bf16(ret.at[1, core], rin.at[1, 0])
            y_save.start()

        @at(st, 3 * num_loc, on_core=0)
        def _():
            far_arrived(1)

        sel, gate = pick(pos, gate_rows, 1, st, cap)
        x = dot(sel, xs[1, block]).astype(BF16)
        for t in range(tiles):
            cols = slice(t * TILE, (t + 1) * TILE)
            a = dot(x, win[e, :, cols])
            b = dot(x, wup[e, :, cols])
            wide_buf[0, t, 0] = (a * jax.nn.sigmoid(a) * b).astype(BF16)
        hid = jnp.concatenate([wide_buf[0, t, 0] for t in range(tiles)], axis=1)
        rows[e] = (gate * dot(hid, wout[e])).astype(BF16)

        finish_block(1, st, range(4))

        return carry

    lax.fori_loop(0, steps, forward_step, 0)
    back(1, 1).wait_recv()
    ret[1, 2 + core] = add_bf16(ret.at[1, 2 + core], rin.at[1, 1])
    yx_save.start()
    back(0, 0).wait_recv()
    dx_cross.wait_recv()
    ret[0, core] = add_bf16(ret.at[0, core], rin.at[0, 0], cin)
    dx_save.start()

    for copy in outs(steps - 1):
        copy.wait()
    for flip in range(4):
        for k in range(2):
            meta(flip, k).wait_send()
    for mb in range(2):
        for k in range(PARTS):
            hop(mb, k).wait_send()
            near(mb, k).wait_send()
            cross(mb, k).wait_send()
            far(mb, k).wait_send()
        for k in range(2):
            back(mb, k).wait_send()
    for copy in (dy_near, dy_cross, dy_far, dx_cross):
        copy.wait_send()
    for copy in (y_save, yx_save, dx_save):
        copy.wait()


def stage_call(num_stages, cap, ids, gates, x_acts, d_out, w_in, w_up, w_out):
    _, num_loc, model, width = w_in.shape
    tokens = x_acts.shape[2]
    slots = 4 * cap
    whole = pl.BlockSpec(memory_space=pltpu.VMEM)
    anyspace = pl.BlockSpec(memory_space=pl.ANY)
    block = jax.ShapeDtypeStruct((tokens, model), BF16)
    wide = jax.ShapeDtypeStruct((num_loc, width // TILE, 3, slots, TILE), BF16)
    tall = jax.ShapeDtypeStruct((num_loc, 2, model, slots), BF16)
    vmem = pltpu.VMEM
    dma = pltpu.SemaphoreType.DMA
    return pl.pallas_call(
        functools.partial(stage_kernel, num_stages, cap),
        out_shape=[block] * 3 + [wide, tall],
        in_specs=[whole] * 2 + [anyspace] * 5,
        out_specs=[anyspace] * 5,
        scratch_shapes=[
            vmem((4,) + ids.shape, jnp.int32), vmem((4,) + gates.shape, F32),
            vmem((2, 4, tokens, model), BF16), vmem((4, tokens, model), BF16),
            vmem((num_loc, model, width), BF16), vmem((num_loc, model, width), BF16),
            vmem((num_loc, width, model), BF16),
            vmem((2, 4 * num_loc, tokens), jnp.int32), vmem((2, 4 * num_loc, tokens), F32),
            vmem((2, tokens, 128), jnp.int32),
            vmem((num_loc, cap, model), BF16), vmem((2, 4, tokens, model), BF16),
            vmem((2, 2, tokens, model), BF16), vmem((tokens, model), BF16),
            vmem((2, width // TILE, 3, cap, TILE), BF16), vmem((2, 2, model, cap), BF16),
            vmem((EARLY, cap, model), BF16), vmem((EARLY, cap, width), F32),
            dma((2, 4)), dma((2, 4)), dma((2, PARTS)), dma((2, PARTS)), dma((2, 3, PARTS)), dma((2, 3, PARTS)),
            dma, dma((3,)), dma((3,)), dma((2, 2)), dma((2, 2)), dma, dma, dma((3,)), dma((2, 2)), dma((3,)),
            pltpu.SemaphoreType.REGULAR,
        ],
        compiler_params=pltpu.CompilerParams(collective_id=0, has_side_effects=True, vmem_limit_bytes=66_500_000),
        cost_estimate=pl.CostEstimate(flops=16 * num_loc * slots * model * width,
                                      bytes_accessed=70 * 2 ** 20, transcendentals=0),
        name='stage_layer',
    )(ids, gates, x_acts, d_out, w_in, w_up, w_out)


def weight_kernel(tall, wide, din_ref, dup_ref, dout_ref):
    for e in range(tall.shape[0]):
        din_ref[e] = dot(tall[e, 0], wide[e, 0, 0]).astype(BF16)
        dup_ref[e] = dot(tall[e, 0], wide[e, 0, 1]).astype(BF16)
        dout_ref[e] = dot(tall[e, 1], wide[e, 0, 2]).T.astype(BF16)


def weight_call(wide, tall):
    num_loc, tiles, _, slots, _ = wide.shape
    model, width = tall.shape[2], tiles * TILE
    return pl.pallas_call(
        weight_kernel,
        grid=(tiles,),
        in_specs=[pl.BlockSpec(tall.shape, lambda t: (0, 0, 0, 0)),
                  pl.BlockSpec((num_loc, 1, 3, slots, TILE), lambda t: (0, t, 0, 0, 0))],
        out_specs=[pl.BlockSpec((num_loc, model, TILE), lambda t: (0, 0, t))] * 2
        + [pl.BlockSpec((num_loc, TILE, model), lambda t: (0, t, 0))],
        out_shape=[jax.ShapeDtypeStruct((num_loc, model, width), BF16)] * 2
        + [jax.ShapeDtypeStruct((num_loc, width, model), BF16)],
        compiler_params=pltpu.CompilerParams(dimension_semantics=('arbitrary',)),
        cost_estimate=pl.CostEstimate(flops=6 * num_loc * slots * model * width,
                                      bytes_accessed=50 * 2 ** 20, transcendentals=0),
        name='weight_grads',
    )(tall, wide)


def solution(mesh):
    group = mesh.shape['expert']
    stages = mesh.shape['stage']

    def device_fn(x_acts, expert_ids, gate_wts, w_in, w_up, w_out, d_out):
        num_loc = w_in.shape[1]
        tokens = x_acts.shape[2]
        top_k = expert_ids.shape[3]
        cap = 3 * top_k * tokens // (2 * num_loc * group)
        ids = jnp.swapaxes(expert_ids[:, 0], 1, 2)
        gates = jnp.swapaxes(gate_wts[:, 0], 1, 2)
        dx_home, y_loc, y_x, wide, tall = stage_call(
            stages, cap, ids, gates, x_acts, d_out, w_in, w_up, w_out)
        d_x = lax.ppermute(dx_home, 'stage', [((s + 1) % stages, s) for s in range(stages)])
        y_in = lax.ppermute(y_x, 'expert', [(i, i ^ 2) for i in range(group)])
        d_in, d_up, d_wout = weight_call(wide, tall)
        y = (y_loc.astype(F32) + y_in.astype(F32)).astype(BF16)
        return y[None], d_x[None], d_in[None], d_up[None], d_wout[None]

    tok_spec = P(None, 'stage', 'expert', None)
    w_spec = P('stage', 'expert', None, None)
    row_spec = P('stage', 'expert', None)
    return jax.shard_map(device_fn, mesh=mesh,
                         in_specs=(tok_spec, tok_spec, tok_spec, w_spec, w_spec, w_spec, row_spec),
                         out_specs=(row_spec, row_spec, w_spec, w_spec, w_spec), check_vma=False)
```
